256 devices in a mesh: comp: 2 (over core), space: 64 (over x, y_hi, z), trc: 2 (over y_lo).
Axes of the slice: x: 4, y: 4 (y_hi: 2, y_lo: 2; y = y_hi * 2 + y_lo), z: 8, core: 2. Of those that a mesh axis runs over, the one named last changes fastest.
Arguments:
- tracers: float32 [16, 8, 512, 1024], P(('comp', 'trc'), None, 'space'), may hold values from -6 to 6
- flow: float32 [16, 512, 1024], P(('comp', 'trc'), 'space'), may hold values from -4 to 4
- reaction_rates: float32 [16, 16], replicated, may hold values from -1.5 to 1.5
- land_mask: int32 [512, 1024], P('space'), may hold values 0 or 1
- layers: int32 [512, 1024], P('space'), may hold values from 1 to 8
Outputs:
- tracers_out: float32 [16, 8, 512, 1024], P(('comp', 'trc'), None, 'space')
- flow_out: float32 [16, 512, 1024], P(('comp', 'trc'), 'space')
The draws below stay inside these ranges and needn't reach their ends.
All inputs are finite; a program needn't handle non-finite values. No bound on the sum of `land_mask` on one device may be relied on, other than what follows from the above.
Results may differ from the reference program's by a relative error of at most 0.0003.
Values sent between devices are 32-bit elements; how exact they have to be, the bound alone decides.
A program may use at most 64 MiB of HBM per device.

```python
import jax
import jax.numpy as jnp
from jax import lax

NTR = 16
NZ = 8
STEPS = 2
NY = 1024
NX = 512


def place_ends(drawn, own_key, low, top_value):
    place = [jax.random.randint(jax.random.fold_in(own_key, axis), (), 0, length) for axis, length in enumerate(drawn.shape)]
    longest = drawn.shape.index(max(drawn.shape))
    next_to = place[:longest] + [(place[longest] + 1) % drawn.shape[longest]] + place[longest + 1:]
    return drawn.at[tuple(place)].set(low).at[tuple(next_to)].set(top_value)


def level_of(own_key, dims, shards, least, top_value):
    def one(dim, blocks):
        heights = jax.random.uniform(jax.random.fold_in(jax.random.fold_in(own_key, 6), dim), (blocks,), jnp.float32, least / len(shards), top_value / len(shards))
        return jnp.repeat(jnp.exp(heights), dims[dim] // blocks).reshape((-1,) + (1,) * (len(dims) - dim - 1))

    factor_of = one(*shards[0])
    for cut in shards[1:]:
        factor_of = factor_of * one(*cut)
    return factor_of


def gaussian(key, shape, scale, reach, shards=(), kind=jnp.bfloat16):
    array = jax.random.normal(key, shape, jnp.float32) * scale
    if len(shards) > 0:
        array = level_of(key, shape, shards, -0.22, 0.18) * array
    return jnp.clip(array, min=-reach, max=reach).astype(kind)


def setup_inputs(seed: int = 0) -> dict:
    splits = jax.random.split(jax.random.key(seed), 6)
    return {
        "tracers": gaussian(splits[0], (NTR, NZ, NX, NY), 1.0, 6.0, ((0, 4), (2, 64)), jnp.float32),
        "flow": gaussian(splits[1], (2 * NZ, NX, NY), 1.0, 4.0, ((0, 4), (1, 64)), jnp.float32),
        "reaction_rates": gaussian(splits[2], (NTR, NTR), NTR ** -0.5, 1.5, (), jnp.float32),
        "land_mask": place_ends((jax.random.randint(splits[3], (NX, NY), 0, 5) < 4).astype(jnp.int32), jax.random.fold_in(splits[3], 1), 0, 1),
        "layers": place_ends(jax.random.randint(splits[4], (NX, NY), 1, NZ + 1), jax.random.fold_in(splits[4], 1), 1, NZ).astype(jnp.int32),
    }


courant = 0.25
viscosity = 0.2
coriolis = 0.3
friction = 0.1
diffusion = 0.3
react_step = 0.5


def trimmed(values, front, back, along):
    along = along % values.ndim
    return lax.slice_in_dim(values, front, values.shape[along] - back, axis=along)


def padded(values, width, along):
    along = along % values.ndim
    spec = [(0, 0)] * values.ndim
    spec[along] = (width, width)
    return jnp.pad(values, spec)


def minmod(first, second):
    return 0.5 * (jnp.sign(first) + jnp.sign(second)) * jnp.minimum(jnp.abs(first), jnp.abs(second))


def sweep(field, speed, wetness, along):
    jumps = trimmed(field, 1, 0, along) - trimmed(field, 0, 1, along)
    slopes = minmod(trimmed(jumps, 0, 1, along), trimmed(jumps, 1, 0, along))
    faces = 0.5 * (trimmed(speed, 0, 1, along) + trimmed(speed, 1, 0, along)) * trimmed(wetness, 0, 1, along) * trimmed(wetness, 1, 0, along)
    upper = jnp.maximum(faces, 0.0)
    lower = jnp.minimum(faces, 0.0)
    fluxes = upper * (trimmed(field, 1, 2, along) + 0.5 * (1.0 - courant * upper) * trimmed(slopes, 0, 1, along)) + lower * (trimmed(field, 2, 1, along) - 0.5 * (1.0 + courant * lower) * trimmed(slopes, 1, 0, along))
    return -courant * (trimmed(fluxes, 1, 0, along) - trimmed(fluxes, 0, 1, along))


def tendency(field, east, north, wetness):
    across = sweep(field, east, wetness, -2)
    inner = trimmed(field, 2, 2, -2)
    north_in = trimmed(north, 1, 1, -2)
    wet_in = trimmed(wetness, 1, 1, -2)
    return across + sweep(padded(inner, 2, -1), padded(north_in, 1, -1), padded(wet_in, 1, -1), -1)


def mixing(field, wetness):
    flows = diffusion * trimmed(wetness, 1, 0, -3) * trimmed(wetness, 0, 1, -3) * (trimmed(field, 1, 0, -3) - trimmed(field, 0, 1, -3))
    edged = padded(flows, 1, -3)
    return field + (trimmed(edged, 1, 0, -3) - trimmed(edged, 0, 1, -3))


def laplace(ghosted):
    widened = padded(ghosted, 1, -1)
    center = widened[:, 1:-1, 1:-1]
    return widened[:, 2:, 1:-1] + widened[:, :-2, 1:-1] + widened[:, 1:-1, 2:] + widened[:, 1:-1, :-2] - 4.0 * center


def react(field, rates):
    flat = field.reshape(field.shape[0], -1)
    soft = flat / (1.0 + jnp.abs(flat))
    return field + react_step * jnp.dot(rates, soft, precision=lax.Precision.HIGHEST).reshape(field.shape)


def wet_cells(land_mask, layers, depth):
    levels = lax.broadcasted_iota(jnp.int32, (depth,) + land_mask.shape, 0)
    return jnp.where((levels < layers[None]) & (land_mask[None] > 0), 1.0, 0.0).astype(jnp.float32)


def reference(tracers, flow, reaction_rates, land_mask, layers):
    wetness = wet_cells(land_mask, layers, NZ)
    wet_pad = padded(wetness, 1, -2)
    east_flow = flow[:NZ]
    north_flow = flow[NZ:]
    for step_index in range(STEPS):
        east_new = wetness * (east_flow + coriolis * north_flow + viscosity * laplace(padded(east_flow, 1, -2)) - friction * east_flow)
        north_new = wetness * (north_flow + (-coriolis) * east_flow + viscosity * laplace(padded(north_flow, 1, -2)) - friction * north_flow)
        east_flow = east_new
        north_flow = north_new
        east_pad = padded(east_flow, 1, -2)
        north_pad = padded(north_flow, 1, -2)

        def advance(column):
            first = column + tendency(padded(column, 2, -2), east_pad, north_pad, wet_pad)
            second = 0.5 * ((column + first) + tendency(padded(first, 2, -2), east_pad, north_pad, wet_pad))
            return mixing(second, wetness)

        tracers = lax.map(advance, tracers)
        tracers = react(tracers, reaction_rates)
    return tracers, jnp.concatenate([east_flow, north_flow], 0)
```

```python
import functools

import jax
import jax.numpy as jnp
from jax import lax
from jax.experimental import pallas as pl
from jax.experimental.pallas import tpu as pltpu
from jax.sharding import PartitionSpec as P

STEPS = 2
COURANT = 0.25
VISCOSITY = 0.2
CORIOLIS = 0.3
FRICTION = 0.1
DIFFUSION = 0.3
REACT_STEP = 0.5

MESH = pl.DeviceIdType.MESH
F32 = jnp.float32
ROWS = 8
DEEP = 24
GHOST = 4
SPAN = ROWS + 2 * GHOST
PAIR = 256


def limited(before, after):
    return jnp.maximum(jnp.minimum(after, 0.0), jnp.minimum(before, jnp.maximum(after, 0.0)))


def roll_lanes(a, by):
    return pltpu.roll(a, by % a.shape[-1], a.ndim - 1)


def kernel(
    tracers, flow, land, layers, matrix, out, flow_out,
    tr_v, fl_v, dep_v, stage, grid, first, part, second, coef_x, coef_y, mix_w, natural,
    field, depth_v, packed, ext, final, velocity_send,
    in_local, in_sem_s, in_sem_r, fl_local, fl_sem_s, fl_sem_r, dep_s, dep_r,
    halo_s, halo_r, mix_s, mix_r, out_s, out_r, own_out, fo_s, fo_r, fo_own,
):
    ny = tracers.shape[-1]
    c = lax.axis_index("comp")
    sp = lax.axis_index("space")
    t = lax.axis_index("trc")
    n = lax.axis_size("space")
    v = 2 * t + c
    w = 2 * c + t
    has_prev = sp > 0
    has_next = sp < n - 1

    def at(cc, ss, tt):
        return {"comp": cc, "space": ss, "trc": tt}

    def remote(src, dst, s, r, dev):
        return pltpu.make_async_remote_copy(
            src_ref=src, dst_ref=dst, send_sem=s, recv_sem=r, device_id=dev, device_id_type=MESH
        )

    my_flow = pltpu.make_async_copy(
        flow.at[pl.ds(2 * c, 2)], field.at[0, c, :, pl.ds(ROWS, ROWS)], fl_local.at[0]
    )
    all_flow = pltpu.make_async_copy(flow, fl_v, fl_local.at[1])
    all_tr = pltpu.make_async_copy(tracers, tr_v, in_local.at[0])
    own_tr = [
        pltpu.make_async_copy(tracers.at[:, 2 * v + e], stage.at[w, e], in_local.at[1 + e])
        for e in range(2)
    ]
    all_tr.start()
    all_flow.start()
    my_flow.start()
    for copy in own_tr:
        copy.start()

    barrier = pltpu.get_barrier_semaphore()
    peers = [(c, 1 - t), (1 - c, 1 - t), (1 - c, t)]
    for cc, tt in peers:
        pl.semaphore_signal(barrier, inc=1, device_id=at(cc, sp, tt), device_id_type=MESH)

    @pl.when(has_prev)
    def _():
        for cc in range(2):
            pl.semaphore_signal(barrier, inc=1, device_id=at(cc, sp - 1, t), device_id_type=MESH)

    @pl.when(has_next)
    def _():
        for cc in range(2):
            pl.semaphore_signal(barrier, inc=1, device_id=at(cc, sp + 1, t), device_id_type=MESH)

    dep_v[...] = jnp.where(land[...] > 0, layers[...], 0).astype(F32)
    depth_v[ROWS : 2 * ROWS] = dep_v[...]

    @pl.when(jnp.logical_not(has_prev))
    def _():
        depth_v[0:ROWS] = jnp.zeros((ROWS, ny), F32)
        for comp in range(2):
            for e in range(2):
                field[0, comp, e, 0:ROWS] = jnp.zeros((ROWS, ny), F32)
        for step in range(2):
            for slot in range(4):
                for row in range(GHOST):
                    grid[step, slot, row] = jnp.zeros((8, ny), F32)

    @pl.when(jnp.logical_not(has_next))
    def _():
        depth_v[2 * ROWS :] = jnp.zeros((ROWS, ny), F32)
        for comp in range(2):
            for e in range(2):
                field[0, comp, e, 2 * ROWS :] = jnp.zeros((ROWS, ny), F32)
        for step in range(2):
            for slot in range(4):
                for row in range(GHOST):
                    grid[step, slot, GHOST + ROWS + row] = jnp.zeros((8, ny), F32)

    @pl.when(v == 0)
    def _():
        for step in range(2):
            for p in range(2):
                ext[step, 0, p] = jnp.zeros((ROWS, 8, ny), F32)

    @pl.when(v == 3)
    def _():
        for step in range(2):
            for p in range(2):
                ext[step, 1, p] = jnp.zeros((ROWS, 8, ny), F32)

    pl.semaphore_wait(
        barrier, 3 + 2 * jnp.where(has_prev, 1, 0) + 2 * jnp.where(has_next, 1, 0)
    )

    def in_copy(k, e):
        cc, tt = peers[k]
        return remote(
            tr_v.at[:, 2 * (2 * tt + cc) + e], stage.at[w, e],
            in_sem_s.at[k, e], in_sem_r.at[w, e], at(cc, sp, tt),
        )

    all_tr.wait()
    for k in (2, 0, 1):
        for e in range(2):
            in_copy(k, e).start()

    def flow_copy(d, cc):
        return remote(
            fl_v.at[pl.ds(2 * cc, 2)],
            field.at[0, c, :, pl.ds(ROWS * (1 - d), ROWS)],
            fl_sem_s.at[d + 1, cc], fl_sem_r.at[1 - d, c], at(cc, sp + d, t),
        )

    def dep_copy(d):
        return remote(
            dep_v, depth_v.at[pl.ds(ROWS * (1 - d), ROWS)],
            dep_s.at[d + 1], dep_r.at[1 - d], at(c, sp + d, t),
        )

    partner_flow = remote(
        fl_v.at[pl.ds(2 * (1 - c), 2)], field.at[0, c, :, pl.ds(ROWS, ROWS)],
        fl_sem_s.at[1, 0], fl_sem_r.at[1, 0], at(1 - c, sp, t),
    )
    all_flow.wait()
    partner_flow.start()

    @pl.when(has_prev)
    def _():
        dep_copy(-1).start()
        for cc in range(2):
            flow_copy(-1, cc).start()

    @pl.when(has_next)
    def _():
        dep_copy(1).start()
        for cc in range(2):
            flow_copy(1, cc).start()

    def halo_copy(step, slot, d):
        low = d < 0
        return remote(
            grid.at[step, slot, pl.ds(GHOST if low else ROWS, GHOST)],
            grid.at[step, slot, pl.ds(GHOST + ROWS if low else 0, GHOST)],
            halo_s.at[step, slot, 0 if low else 1], halo_r.at[step, slot, 1 if low else 0],
            at(c, sp + d, t),
        )

    def halo_start(step, slot):
        @pl.when(has_prev)
        def _():
            halo_copy(step, slot, -1).start()

        @pl.when(has_next)
        def _():
            halo_copy(step, slot, 1).start()

    def halo_wait(step, slot):
        @pl.when(has_prev)
        def _():
            halo_copy(step, slot, 1).wait_recv()

        @pl.when(has_next)
        def _():
            halo_copy(step, slot, -1).wait_recv()

    def halo_sent(step, slot):
        @pl.when(has_prev)
        def _():
            halo_copy(step, slot, -1).wait_send()

        @pl.when(has_next)
        def _():
            halo_copy(step, slot, 1).wait_send()

    def regroup(slot):
        def tile(q, _):
            lanes = pl.ds(pl.multiple_of(q * 128, 128), 128)
            x = stage[slot, :, :, :, lanes].reshape(8, ROWS, 128)
            grid[0, slot, pl.ds(GHOST, ROWS), :, lanes] = jnp.swapaxes(x, 0, 1)
            return 0

        lax.fori_loop(0, ny // 128, tile, 0)

    def arrived(k):
        cc, tt = peers[k]
        slot = 2 * cc + tt
        for e in range(2):
            remote(
                stage.at[slot, e], stage.at[slot, e], in_sem_s.at[k, e], in_sem_r.at[slot, e],
                at(cc, sp, tt),
            ).wait_recv()
        regroup(slot)
        halo_start(0, slot)

    for copy in own_tr:
        copy.wait()
    regroup(w)
    halo_start(0, w)
    arrived(2)

    my_flow.wait()
    partner_flow.wait_recv()

    @pl.when(has_prev)
    def _():
        dep_copy(1).wait_recv()
        for cc in range(2):
            remote(
                fl_v.at[pl.ds(0, 2)], field.at[0, cc, :, pl.ds(0, ROWS)],
                fl_sem_s.at[0, cc], fl_sem_r.at[0, cc], at(cc, sp - 1, t),
            ).wait_recv()

    @pl.when(has_next)
    def _():
        dep_copy(-1).wait_recv()
        for cc in range(2):
            remote(
                fl_v.at[pl.ds(0, 2)], field.at[0, cc, :, pl.ds(2 * ROWS, ROWS)],
                fl_sem_s.at[2, cc], fl_sem_r.at[2, cc], at(cc, sp + 1, t),
            ).wait_recv()

    lane_deep = lax.broadcasted_iota(jnp.int32, (DEEP, ny), 1)
    top_half = lax.broadcasted_iota(jnp.int32, (8, ny), 0) < 4
    lane = lax.broadcasted_iota(jnp.int32, (8, ny), 1)
    at_first = lane == 0
    at_last = lane == ny - 1

    def wet_of(level, rows):
        return jnp.where(depth_v[rows] > level.astype(F32), 1.0, 0.0)

    def lap(a):
        left = jnp.where(lane_deep == 0, 0.0, roll_lanes(a, 1))
        right = jnp.where(lane_deep == ny - 1, 0.0, roll_lanes(a, -1))
        return pltpu.roll(a, 1, 0) + pltpu.roll(a, DEEP - 1, 0) + left + right - 4.0 * a

    def put_coefs(e, base, face):
        up = jnp.maximum(face, 0.0)
        down = jnp.minimum(face, 0.0)
        natural[e, base] = -COURANT * up
        natural[e, base + 1] = (-COURANT * 0.5) * up * (1.0 - COURANT * up)
        natural[e, base + 2] = -COURANT * down
        natural[e, base + 3] = (COURANT * 0.5) * down * (1.0 + COURANT * down)

    def spread_rows(ref, k, j):
        one = jnp.broadcast_to(ref[0, k, j : j + 1, :], (8, ny))
        two = jnp.broadcast_to(ref[1, k, j : j + 1, :], (8, ny))
        return jnp.where(top_half, one, two)

    def velocities(step, _):
        def level(e, _):
            wet = wet_of(2 * v + e, slice(None))
            u = field[step, 0, e]
            r = field[step, 1, e]
            u_new = wet * (u + CORIOLIS * r + VISCOSITY * lap(u) - FRICTION * u)
            r_new = wet * (r - CORIOLIS * u + VISCOSITY * lap(r) - FRICTION * r)
            field[step + 1, 0, e] = u_new
            field[step + 1, 1, e] = r_new
            face = 0.5 * (u_new + pltpu.roll(u_new, DEEP - 1, 0)) * wet * pltpu.roll(wet, DEEP - 1, 0)
            put_coefs(e, 0, face)
            wet_right = jnp.where(lane_deep == ny - 1, 0.0, roll_lanes(wet, -1))
            face = 0.5 * (r_new + roll_lanes(r_new, -1)) * wet * wet_right
            put_coefs(e, 4, face)
            return 0

        lax.fori_loop(0, 2, level, 0)
        shift = ROWS - GHOST
        for i in range(1, 14):
            for k in range(4):
                coef_x[step, i - 1, k] = spread_rows(natural, k, i + shift)
        for i in range(2, 14):
            for k in range(4):
                coef_y[step, i - 2, k] = spread_rows(natural, 4 + k, i + shift)
        return 0

    lax.fori_loop(0, STEPS, velocities, 0)

    middle = slice(ROWS, 2 * ROWS)
    above = jnp.where(v > 0, DIFFUSION, 0.0).astype(F32)
    wet_a = wet_of(2 * v, middle)
    wet_b = wet_of(2 * v + 1, middle)
    natural[0, 0, 0:ROWS] = DIFFUSION * wet_a * wet_b
    natural[1, 0, 0:ROWS] = DIFFUSION * wet_a * wet_b
    natural[0, 1, 0:ROWS] = above * wet_a * wet_of(2 * v - 1, middle)
    natural[1, 1, 0:ROWS] = DIFFUSION * wet_b * wet_of(2 * v + 2, middle)
    for row in range(ROWS):
        for k in range(2):
            mix_w[row, k] = spread_rows(natural, k, row)

    for e in range(2):
        velocity_send[0, e] = field[STEPS, c, e, ROWS : 2 * ROWS]
        velocity_send[1, e] = field[STEPS, 1 - c, e, ROWS : 2 * ROWS]
    flow_own = pltpu.make_async_copy(velocity_send.at[0], flow_out.at[pl.ds(2 * c, 2)], fo_own.at[0])
    flow_far = remote(
        velocity_send.at[1], flow_out.at[pl.ds(2 * c, 2)], fo_s.at[0], fo_r.at[0], at(1 - c, sp, t)
    )
    flow_own.start()
    flow_far.start()

    def along_x(step, load, first_face, last_face, put):
        def chunk(q, _):
            lanes = pl.ds(pl.multiple_of(q * PAIR, PAIR), PAIR)
            before = load(first_face - 1, lanes)
            here = load(first_face, lanes)
            ahead = load(first_face + 1, lanes)
            jump = ahead - here
            slope = limited(here - before, jump)
            last_flux = None
            for i in range(first_face, last_face + 1):
                far = load(i + 2, lanes)
                next_jump = far - ahead
                next_slope = limited(jump, next_jump)
                k = i - 1
                flux = (
                    coef_x[step, k, 0, :, lanes] * here
                    + coef_x[step, k, 1, :, lanes] * slope
                    + coef_x[step, k, 2, :, lanes] * ahead
                    + coef_x[step, k, 3, :, lanes] * next_slope
                )
                if last_flux is not None:
                    put(i, lanes, here, flux - last_flux)
                last_flux = flux
                here, ahead, jump, slope = ahead, far, next_jump, next_slope
            return 0

        lax.fori_loop(0, ny // PAIR, chunk, 0)

    def along_y(step, i, a):
        right = jnp.where(at_last, 0.0, roll_lanes(a, -1))
        jump = right - a
        slope = limited(jnp.where(at_first, a, roll_lanes(jump, 1)), jump)
        flux = (
            coef_y[step, i - 2, 0] * a
            + coef_y[step, i - 2, 1] * slope
            + coef_y[step, i - 2, 2] * right
            + coef_y[step, i - 2, 3] * roll_lanes(slope, -1)
        )
        return flux - roll_lanes(flux, 1)

    def advance(step, slot):
        def put_one(i, lanes, here, change):
            part[i, :, lanes] = here + change

        along_x(step, lambda i, lanes: grid[step, slot, i, :, lanes], 1, 13, put_one)

        def row_one(i, _):
            first[i] = part[i] + along_y(step, i, grid[step, slot, i])
            return 0

        lax.fori_loop(2, 14, row_one, 0)

        def put_two(i, lanes, here, change):
            part[i, :, lanes] = (grid[step, slot, i, :, lanes] + here) + change

        along_x(step, lambda i, lanes: first[i, :, lanes], 3, 11, put_two)

        def row_two(i, _):
            second[slot, i - GHOST] = 0.5 * (part[i] + along_y(step, i, first[i]))
            return 0

        lax.fori_loop(GHOST, GHOST + ROWS, row_two, 0)

    def swap_halves(a):
        return pltpu.roll(a, 4, 0)

    def mix_copy(step, p, d):
        up = v + d
        return remote(
            packed.at[step, p, 0 if d < 0 else 1], ext.at[step, 1 if d < 0 else 0, p],
            mix_s.at[step, p, 0 if d < 0 else 1], mix_r.at[step, p, 1 if d < 0 else 0],
            at(lax.rem(up, 2), sp, up // 2),
        )

    def mix_start(step, p):
        def row(i, _):
            a = second[p, i]
            b = second[p + 2, i]
            packed[step, p, 0, i] = jnp.where(top_half, a, swap_halves(b))
            packed[step, p, 1, i] = jnp.where(top_half, swap_halves(a), b)
            return 0

        lax.fori_loop(0, ROWS, row, 0)

        @pl.when(v > 0)
        def _():
            mix_copy(step, p, -1).start()

        @pl.when(v < 3)
        def _():
            mix_copy(step, p, 1).start()

    def mix_wait(step, p):
        @pl.when(v > 0)
        def _():
            mix_copy(step, p, 1).wait_recv()

        @pl.when(v < 3)
        def _():
            mix_copy(step, p, -1).wait_recv()

    def mix_sent(step, p):
        @pl.when(v > 0)
        def _():
            mix_copy(step, p, -1).wait_send()

        @pl.when(v < 3)
        def _():
            mix_copy(step, p, 1).wait_send()

    def settle(step, put, rows):
        def row(i, _):
            inner = mix_w[i, 0]
            outer = mix_w[i, 1]
            mixed = [None] * 4
            for p in range(2):
                low = ext[step, 0, p, i]
                high = ext[step, 1, p, i]
                beyond = (
                    jnp.where(top_half, low, swap_halves(high)),
                    jnp.where(top_half, swap_halves(low), high),
                )
                for half in range(2):
                    a = second[p + 2 * half, i]
                    mixed[p + 2 * half] = (
                        a + inner * (swap_halves(a) - a) + outer * (beyond[half] - a)
                    )
            whole = jnp.concatenate(mixed, axis=0)
            soft = whole / (1.0 + jnp.abs(whole))
            done = whole + jnp.dot(
                matrix[...], soft, precision=lax.Precision.HIGHEST, preferred_element_type=F32
            )
            for slot in range(4):
                put(slot, i, done[8 * slot : 8 * slot + 8])
            return 0

        lax.fori_loop(*rows, row, 0)

    def run(step, order):
        own_pair, far_pair = t, 1 - t
        for number, slot in enumerate(order):
            if step == 0 and number >= 2:
                arrived(number - 2)
            halo_wait(step, slot)
            advance(step, slot)
            if number == 1:
                mix_start(step, own_pair)
        mix_start(step, far_pair)
        for p in range(2):
            mix_wait(step, p)

    order = [w, 2 * (1 - c) + t, 2 * c + 1 - t, 2 * (1 - c) + 1 - t]
    run(0, order)

    def put_next(slot, i, a):
        grid[1, slot, GHOST + i] = a

    settle(0, put_next, (0, ROWS))
    for slot in order:
        halo_start(1, slot)
    run(1, order)

    def put_final(slot, i, a):
        final[slot, i] = a

    half = ROWS // 2

    def out_copy(k, h):
        cc, tt = peers[k]
        return remote(
            final.at[2 * cc + tt, pl.ds(half * h, half)], out.at[v, pl.ds(half * h, half)],
            out_s.at[k, h], out_r.at[v, h], at(cc, sp, tt),
        )

    own_copies = []
    for h in range(2):
        settle(1, put_final, (half * h, half * (h + 1)))
        for k in (0, 1, 2):
            out_copy(k, h).start()
        copy = pltpu.make_async_copy(
            final.at[w, pl.ds(half * h, half)], out.at[v, pl.ds(half * h, half)], own_out.at[h]
        )
        copy.start()
        own_copies.append(copy)

    for copy in own_copies:
        copy.wait()
    flow_own.wait()
    flow_far.wait_send()
    remote(
        velocity_send.at[1], flow_out.at[pl.ds(2 * (1 - c), 2)], fo_s.at[0], fo_r.at[0],
        at(1 - c, sp, t),
    ).wait_recv()
    for k in range(3):
        for e in range(2):
            in_copy(k, e).wait_send()
    partner_flow.wait_send()

    @pl.when(has_prev)
    def _():
        dep_copy(-1).wait_send()
        for cc in range(2):
            flow_copy(-1, cc).wait_send()

    @pl.when(has_next)
    def _():
        dep_copy(1).wait_send()
        for cc in range(2):
            flow_copy(1, cc).wait_send()

    for step in range(STEPS):
        for slot in range(4):
            halo_sent(step, slot)
        for p in range(2):
            mix_sent(step, p)
    for k in range(3):
        cc, tt = peers[k]
        source = 2 * tt + cc
        for h in range(2):
            out_copy(k, h).wait_send()
            remote(
                final.at[w, pl.ds(half * h, half)], out.at[source, pl.ds(half * h, half)],
                out_s.at[k, h], out_r.at[source, h], at(cc, sp, tt),
            ).wait_recv()


def place(blocks, flow, out, flow_out):
    x = jnp.swapaxes(blocks[0], 0, 1)
    for e in range(2):
        for s in range(4):
            out[s, e] = x[4 * e + s]

    @pl.when(pl.program_id(0) == 0)
    def _():
        flow_out[...] = flow[...]


def body(tracers, flow, reaction_rates, land_mask, layers):
    ny = tracers.shape[-1]
    rates = REACT_STEP * reaction_rates.reshape(4, 1, 4, 4, 1, 4)
    matrix = (rates * jnp.eye(2, dtype=F32).reshape(1, 2, 1, 1, 2, 1)).reshape(32, 32)
    vmem = pl.BlockSpec(memory_space=pltpu.VMEM)
    anywhere = pl.BlockSpec(memory_space=pl.ANY)
    dma = pltpu.SemaphoreType.DMA
    blocks, flow_done = pl.pallas_call(
        kernel,
        out_shape=(
            jax.ShapeDtypeStruct((4, ROWS, 8, ny), F32),
            jax.ShapeDtypeStruct((4, ROWS, ny), F32),
        ),
        in_specs=[anywhere, anywhere, vmem, vmem, vmem],
        out_specs=(anywhere, anywhere),
        scratch_shapes=[
            pltpu.VMEM((4, 8, ROWS, ny), F32),
            pltpu.VMEM((4, ROWS, ny), F32),
            pltpu.VMEM((ROWS, ny), F32),
            pltpu.VMEM((4, 2, 4, ROWS, ny), F32),
            pltpu.VMEM((STEPS, 4, SPAN, 8, ny), F32),
            pltpu.VMEM((SPAN, 8, ny), F32),
            pltpu.VMEM((SPAN, 8, ny), F32),
            pltpu.VMEM((4, ROWS, 8, ny), F32),
            pltpu.VMEM((STEPS, 13, 4, 8, ny), F32),
            pltpu.VMEM((STEPS, 12, 4, 8, ny), F32),
            pltpu.VMEM((ROWS, 2, 8, ny), F32),
            pltpu.VMEM((2, 8, DEEP, ny), F32),
            pltpu.VMEM((STEPS + 1, 2, 2, DEEP, ny), F32),
            pltpu.VMEM((DEEP, ny), F32),
            pltpu.VMEM((STEPS, 2, 2, ROWS, 8, ny), F32),
            pltpu.VMEM((STEPS, 2, 2, ROWS, 8, ny), F32),
            pltpu.VMEM((4, ROWS, 8, ny), F32),
            pltpu.VMEM((2, 2, ROWS, ny), F32),
            dma((3,)), dma((3, 2)), dma((4, 2)),
            dma((2,)), dma((3, 2)), dma((3, 2)), dma((3,)), dma((3,)),
            dma((STEPS, 4, 2)), dma((STEPS, 4, 2)),
            dma((STEPS, 2, 2)), dma((STEPS, 2, 2)),
            dma((3, 2)), dma((4, 2)), dma((2,)),
            dma((1,)), dma((1,)), dma((1,)),
        ],
        compiler_params=pltpu.CompilerParams(
            collective_id=0, has_side_effects=True, vmem_limit_bytes=48 * 1024 * 1024
        ),
        name="ocean",
    )(tracers, flow, land_mask, layers, matrix)
    return pl.pallas_call(
        place,
        grid=(4,),
        out_shape=(
            jax.ShapeDtypeStruct(tracers.shape, F32),
            jax.ShapeDtypeStruct(flow.shape, F32),
        ),
        in_specs=[
            pl.BlockSpec((1, ROWS, 8, ny), lambda g: (g, 0, 0, 0)),
            pl.BlockSpec((4, ROWS, ny), lambda g: (0, 0, 0)),
        ],
        out_specs=(
            pl.BlockSpec((4, 2, ROWS, ny), lambda g: (0, g, 0, 0)),
            pl.BlockSpec((4, ROWS, ny), lambda g: (0, 0, 0)),
        ),
        name="place",
    )(blocks, flow_done)


def solution(mesh):
    placed = (
        P(("comp", "trc"), None, "space", None),
        P(("comp", "trc"), "space", None),
        P(),
        P("space", None),
        P("space", None),
    )
    return jax.shard_map(
        body,
        mesh=mesh,
        in_specs=placed,
        out_specs=(P(("comp", "trc"), None, "space", None), P(("comp", "trc"), "space", None)),
        check_vma=False,
    )
```

```python
import functools

import jax
import jax.numpy as jnp
from jax import lax
from jax.experimental import pallas as pl
from jax.experimental.pallas import tpu as pltpu
from jax.sharding import PartitionSpec as P

STEPS = 2
COURANT = 0.25
VISCOSITY = 0.2
CORIOLIS = 0.3
FRICTION = 0.1
DIFFUSION = 0.3
REACT_STEP = 0.5

MESH = pl.DeviceIdType.MESH
F32 = jnp.float32
ROWS = 8
DEEP = 24
GHOST = 4
SPAN = ROWS + 2 * GHOST
HALF = ROWS // 2
ALL_VMEM = 67_043_328
LINE = 8
PAIR = 256


def limited(before, after):
    return jnp.maximum(jnp.minimum(after, 0.0), jnp.minimum(before, jnp.maximum(after, 0.0)))


def roll_lanes(a, by):
    return pltpu.roll(a, by % a.shape[-1], a.ndim - 1)


def kernel(
    tracers, flow, rates, land, layers, out, flow_out,
    tr_v, fl_v, dep_v, matrix, stage, grid, first, part, second, coef_x, coef_y, mix_w, natural,
    field, depth_v, packed, ext, final, velocity_send,
    in_local, in_sem_s, in_sem_r, fl_local, fl_sem_s, fl_sem_r, rel_s, rel_r, dep_s, dep_r,
    halo_s, halo_r, mix_s, mix_r, out_s, out_r, own_out, fo_s, fo_r, fo_own,
):
    ny = tracers.shape[-1]
    c = lax.axis_index("comp")
    sp = lax.axis_index("space")
    t = lax.axis_index("trc")
    n = lax.axis_size("space")
    w = 2 * c + t
    has_prev = sp > 0
    has_next = sp < n - 1

    def odd(strip):
        return lax.rem(strip // LINE, 2)

    def flipped(bit, strip):
        return lax.rem(bit + odd(strip), 2)

    flip = odd(sp)
    tl = flipped(t, sp)
    v = 2 * tl + c

    def at(cc, ss, tt):
        return {"comp": cc, "space": ss, "trc": tt}

    def holder(pair, strip):
        return at(lax.rem(pair, 2), strip, flipped(pair // 2, strip))

    def remote(src, dst, s, r, dev):
        return pltpu.make_async_remote_copy(
            src_ref=src, dst_ref=dst, send_sem=s, recv_sem=r, device_id=dev, device_id_type=MESH
        )

    middle = pl.ds(ROWS, ROWS)

    all_flow = pltpu.make_async_copy(flow, fl_v, fl_local.at[1])
    all_tr = pltpu.make_async_copy(tracers, tr_v, in_local.at[0])
    own_tr = [
        pltpu.make_async_copy(tracers.at[:, 2 * v + e], stage.at[w, e], in_local.at[1 + e])
        for e in range(2)
    ]
    my_flow = pltpu.make_async_copy(
        flow.at[pl.ds(2 * c, 2)], field.at[0, c, :, middle], fl_local.at[0]
    )
    all_flow.start()
    all_tr.start()
    for copy in own_tr:
        copy.start()

    @pl.when(flip == 0)
    def _():
        my_flow.start()

    barrier = pltpu.get_barrier_semaphore()
    peers = [(c, 1 - t), (1 - c, 1 - t), (1 - c, t)]

    def pair_of(cc, tt):
        return 2 * flipped(tt, sp) + cc

    for cc, tt in peers:
        pl.semaphore_signal(barrier, inc=1, device_id=at(cc, sp, tt), device_id_type=MESH)

    @pl.when(has_prev)
    def _():
        pl.semaphore_signal(barrier, inc=1, device_id=holder(v, sp - 1), device_id_type=MESH)

    @pl.when(has_next)
    def _():
        pl.semaphore_signal(barrier, inc=1, device_id=holder(v, sp + 1), device_id_type=MESH)

    dep_v[...] = jnp.where(land[...] > 0, layers[...], 0).astype(F32)
    depth_v[middle] = dep_v[...]

    @pl.when(jnp.logical_not(has_prev))
    def _():
        depth_v[0:ROWS] = jnp.zeros((ROWS, ny), F32)
        for comp in range(2):
            for e in range(2):
                field[0, comp, e, 0:ROWS] = jnp.zeros((ROWS, ny), F32)
        for step in range(2):
            for slot in range(4):
                for row in range(GHOST):
                    grid[step, slot, row] = jnp.zeros((8, ny), F32)

    @pl.when(jnp.logical_not(has_next))
    def _():
        depth_v[2 * ROWS :] = jnp.zeros((ROWS, ny), F32)
        for comp in range(2):
            for e in range(2):
                field[0, comp, e, 2 * ROWS :] = jnp.zeros((ROWS, ny), F32)
        for step in range(2):
            for slot in range(4):
                for row in range(GHOST):
                    grid[step, slot, GHOST + ROWS + row] = jnp.zeros((8, ny), F32)

    @pl.when(v == 0)
    def _():
        for step in range(2):
            for slot in range(4):
                ext[step, 0, slot] = jnp.zeros((HALF, 8, ny), F32)

    @pl.when(v == 3)
    def _():
        for step in range(2):
            for slot in range(4):
                ext[step, 1, slot] = jnp.zeros((HALF, 8, ny), F32)

    lines = lax.broadcasted_iota(jnp.int32, (32, 16), 0)
    names = lax.broadcasted_iota(jnp.int32, (32, 16), 1)
    pick = jnp.where(4 * (lines // 8) + lax.rem(lines, 4) == names, 1.0, 0.0)
    wide = jnp.dot(pick, rates[...], precision=lax.Precision.HIGHEST, preferred_element_type=F32)
    wide = lax.dot_general(
        wide, pick, (((1,), (1,)), ((), ())),
        precision=lax.Precision.HIGHEST, preferred_element_type=F32,
    )
    line = lax.broadcasted_iota(jnp.int32, (32, 32), 0)
    other = lax.broadcasted_iota(jnp.int32, (32, 32), 1)
    same_level = lax.rem(line // 4, 2) == lax.rem(other // 4, 2)
    matrix[...] = jnp.where(same_level, REACT_STEP * wide, 0.0)

    all_flow.wait()
    pl.semaphore_wait(barrier, 3 + jnp.where(has_prev, 1, 0) + jnp.where(has_next, 1, 0))

    def flow_copy(cc):
        return remote(
            fl_v.at[pl.ds(2 * cc, 2)], field.at[0, c, :, middle],
            fl_sem_s.at[cc], fl_sem_r.at[c], holder(2 * t + cc, sp),
        )

    def flow_from(cc):
        return remote(
            fl_v.at[pl.ds(0, 2)], field.at[0, cc, :, middle],
            fl_sem_s.at[cc], fl_sem_r.at[cc], at(cc, sp, tl),
        )

    @pl.when(flip == 0)
    def _():
        flow_copy(1 - c).start()

    @pl.when(flip == 1)
    def _():
        for cc in range(2):
            flow_copy(cc).start()

    def in_copy(k, e):
        cc, tt = peers[k]
        return remote(
            tr_v.at[:, 2 * pair_of(cc, tt) + e], stage.at[w, e],
            in_sem_s.at[k, e], in_sem_r.at[w, e], at(cc, sp, tt),
        )

    all_tr.wait()
    for k in (2, 0, 1):
        for e in range(2):
            in_copy(k, e).start()

    def dep_copy(d):
        return remote(
            dep_v, depth_v.at[pl.ds(ROWS * (1 - d), ROWS)],
            dep_s.at[d + 1], dep_r.at[1 - d], holder(v, sp + d),
        )

    def relay_copy(d):
        return remote(
            field.at[0, :, :, middle], field.at[0, :, :, pl.ds(ROWS * (1 - d), ROWS)],
            rel_s.at[d + 1], rel_r.at[1 - d], holder(v, sp + d),
        )

    @pl.when(has_prev)
    def _():
        dep_copy(-1).start()

    @pl.when(has_next)
    def _():
        dep_copy(1).start()

    def halo_copy(step, slot, d):
        low = d < 0
        return remote(
            grid.at[step, slot, pl.ds(GHOST if low else ROWS, GHOST)],
            grid.at[step, slot, pl.ds(GHOST + ROWS if low else 0, GHOST)],
            halo_s.at[step, slot, 0 if low else 1], halo_r.at[step, slot, 1 if low else 0],
            holder(v, sp + d),
        )

    def halo_start(step, slot):
        @pl.when(has_prev)
        def _():
            halo_copy(step, slot, -1).start()

        @pl.when(has_next)
        def _():
            halo_copy(step, slot, 1).start()

    def halo_wait(step, slot):
        @pl.when(has_prev)
        def _():
            halo_copy(step, slot, 1).wait_recv()

        @pl.when(has_next)
        def _():
            halo_copy(step, slot, -1).wait_recv()

    def halo_sent(step, slot):
        @pl.when(has_prev)
        def _():
            halo_copy(step, slot, -1).wait_send()

        @pl.when(has_next)
        def _():
            halo_copy(step, slot, 1).wait_send()

    def regroup(slot):
        def tile(q, _):
            lanes = pl.ds(pl.multiple_of(q * 128, 128), 128)
            x = stage[slot, :, :, :, lanes].reshape(8, ROWS, 128)
            grid[0, slot, pl.ds(GHOST, ROWS), :, lanes] = jnp.swapaxes(x, 0, 1)
            return 0

        lax.fori_loop(0, ny // 128, tile, 0, unroll=2)

    def arrived(k):
        cc, tt = peers[k]
        slot = 2 * cc + tt
        for e in range(2):
            remote(
                stage.at[slot, e], stage.at[slot, e], in_sem_s.at[k, e], in_sem_r.at[slot, e],
                at(cc, sp, tt),
            ).wait_recv()
        regroup(slot)
        halo_start(0, slot)

    for copy in own_tr:
        copy.wait()
    regroup(w)

    @pl.when(flip == 0)
    def _():
        my_flow.wait()
        flow_from(1 - c).wait_recv()

    @pl.when(flip == 1)
    def _():
        for cc in range(2):
            flow_from(cc).wait_recv()

    @pl.when(has_prev)
    def _():
        relay_copy(-1).start()

    @pl.when(has_next)
    def _():
        relay_copy(1).start()

    halo_start(0, w)
    arrived(2)

    @pl.when(has_prev)
    def _():
        dep_copy(1).wait_recv()
        relay_copy(1).wait_recv()

    @pl.when(has_next)
    def _():
        dep_copy(-1).wait_recv()
        relay_copy(-1).wait_recv()

    lane_deep = lax.broadcasted_iota(jnp.int32, (DEEP, ny), 1)
    top_half = lax.broadcasted_iota(jnp.int32, (8, ny), 0) < 4
    lane = lax.broadcasted_iota(jnp.int32, (8, ny), 1)
    at_first = lane == 0
    at_last = lane == ny - 1

    def wet_of(level, rows):
        return jnp.where(depth_v[rows] > level.astype(F32), 1.0, 0.0)

    def lap(a):
        left = jnp.where(lane_deep == 0, 0.0, roll_lanes(a, 1))
        right = jnp.where(lane_deep == ny - 1, 0.0, roll_lanes(a, -1))
        return pltpu.roll(a, 1, 0) + pltpu.roll(a, DEEP - 1, 0) + left + right - 4.0 * a

    def put_coefs(e, base, face):
        up = jnp.maximum(face, 0.0)
        down = jnp.minimum(face, 0.0)
        natural[e, base] = -COURANT * up
        natural[e, base + 1] = (-COURANT * 0.5) * up * (1.0 - COURANT * up)
        natural[e, base + 2] = -COURANT * down
        natural[e, base + 3] = (COURANT * 0.5) * down * (1.0 + COURANT * down)

    def spread_rows(ref, k, j):
        one = jnp.broadcast_to(ref[0, k, j : j + 1, :], (8, ny))
        two = jnp.broadcast_to(ref[1, k, j : j + 1, :], (8, ny))
        return jnp.where(top_half, one, two)

    def velocities(step, _):
        def level(e, _):
            wet = wet_of(2 * v + e, slice(None))
            u = field[step, 0, e]
            r = field[step, 1, e]
            u_new = wet * (u + CORIOLIS * r + VISCOSITY * lap(u) - FRICTION * u)
            r_new = wet * (r - CORIOLIS * u + VISCOSITY * lap(r) - FRICTION * r)
            field[step + 1, 0, e] = u_new
            field[step + 1, 1, e] = r_new
            face = 0.5 * (u_new + pltpu.roll(u_new, DEEP - 1, 0)) * wet * pltpu.roll(wet, DEEP - 1, 0)
            put_coefs(e, 0, face)
            wet_right = jnp.where(lane_deep == ny - 1, 0.0, roll_lanes(wet, -1))
            face = 0.5 * (r_new + roll_lanes(r_new, -1)) * wet * wet_right
            put_coefs(e, 4, face)
            return 0

        lax.fori_loop(0, 2, level, 0)
        shift = ROWS - GHOST
        for i in range(1, 14):
            for k in range(4):
                coef_x[step, i - 1, k] = spread_rows(natural, k, i + shift)
        for i in range(2, 14):
            for k in range(4):
                coef_y[step, i - 2, k] = spread_rows(natural, 4 + k, i + shift)
        return 0

    lax.fori_loop(0, STEPS, velocities, 0)

    own_rows = slice(ROWS, 2 * ROWS)
    above = jnp.where(v > 0, DIFFUSION, 0.0).astype(F32)
    wet_a = wet_of(2 * v, own_rows)
    wet_b = wet_of(2 * v + 1, own_rows)
    natural[0, 0, 0:ROWS] = DIFFUSION * wet_a * wet_b
    natural[1, 0, 0:ROWS] = DIFFUSION * wet_a * wet_b
    natural[0, 1, 0:ROWS] = above * wet_a * wet_of(2 * v - 1, own_rows)
    natural[1, 1, 0:ROWS] = DIFFUSION * wet_b * wet_of(2 * v + 2, own_rows)
    for row in range(ROWS):
        for k in range(2):
            mix_w[row, k] = spread_rows(natural, k, row)

    for comp in range(2):
        for e in range(2):
            velocity_send[comp, e] = field[STEPS, comp, e, own_rows]

    def velocity_copy(comp):
        return remote(
            velocity_send.at[comp], flow_out.at[pl.ds(2 * c, 2)],
            fo_s.at[comp], fo_r.at[c], at(comp, sp, tl),
        )

    def velocity_from(cc):
        return remote(
            velocity_send.at[0], flow_out.at[pl.ds(2 * cc, 2)],
            fo_s.at[0], fo_r.at[cc], holder(2 * t + cc, sp),
        )

    velocity_own = pltpu.make_async_copy(
        velocity_send.at[c], flow_out.at[pl.ds(2 * c, 2)], fo_own.at[0]
    )

    @pl.when(flip == 0)
    def _():
        velocity_own.start()
        velocity_copy(1 - c).start()

    @pl.when(flip == 1)
    def _():
        for comp in range(2):
            velocity_copy(comp).start()

    def along_x(step, load, first_face, last_face, put):
        def chunk(q, _):
            lanes = pl.ds(pl.multiple_of(q * PAIR, PAIR), PAIR)
            before = load(first_face - 1, lanes)
            here = load(first_face, lanes)
            ahead = load(first_face + 1, lanes)
            jump = ahead - here
            slope = limited(here - before, jump)
            last_flux = None
            for i in range(first_face, last_face + 1):
                far = load(i + 2, lanes)
                next_jump = far - ahead
                next_slope = limited(jump, next_jump)
                k = i - 1
                flux = (
                    coef_x[step, k, 0, :, lanes] * here
                    + coef_x[step, k, 1, :, lanes] * slope
                    + coef_x[step, k, 2, :, lanes] * ahead
                    + coef_x[step, k, 3, :, lanes] * next_slope
                )
                if last_flux is not None:
                    put(i, lanes, here, flux - last_flux)
                last_flux = flux
                here, ahead, jump, slope = ahead, far, next_jump, next_slope
            return 0

        lax.fori_loop(0, ny // PAIR, chunk, 0)

    def along_y(step, i, a):
        right = jnp.where(at_last, 0.0, roll_lanes(a, -1))
        jump = right - a
        slope = limited(jnp.where(at_first, a, roll_lanes(jump, 1)), jump)
        flux = (
            coef_y[step, i - 2, 0] * a
            + coef_y[step, i - 2, 1] * slope
            + coef_y[step, i - 2, 2] * right
            + coef_y[step, i - 2, 3] * roll_lanes(slope, -1)
        )
        return flux - roll_lanes(flux, 1)

    def advance(step, slot):
        def put_one(i, lanes, here, change):
            part[i, :, lanes] = here + change

        along_x(step, lambda i, lanes: grid[step, slot, i, :, lanes], 1, 13, put_one)

        def row_one(i, _):
            first[i] = part[i] + along_y(step, i, grid[step, slot, i])
            return 0

        lax.fori_loop(2, 14, row_one, 0, unroll=True)

        def put_two(i, lanes, here, change):
            part[i, :, lanes] = (grid[step, slot, i, :, lanes] + here) + change

        along_x(step, lambda i, lanes: first[i, :, lanes], 3, 11, put_two)

        def row_two(i, _):
            second[slot, i - GHOST] = 0.5 * (part[i] + along_y(step, i, first[i]))
            return 0

        lax.fori_loop(GHOST, GHOST + ROWS, row_two, 0, unroll=True)

    def swap_halves(a):
        return pltpu.roll(a, 4, 0)

    def mix_copy(step, slot, d):
        return remote(
            packed.at[step, slot, 0 if d < 0 else 1], ext.at[step, 1 if d < 0 else 0, slot],
            mix_s.at[step, slot, 0 if d < 0 else 1], mix_r.at[step, slot, 1 if d < 0 else 0],
            holder(v + d, sp),
        )

    def mix_start(step, slot):
        def row(i, _):
            a = second[slot, i]
            b = second[slot, i + HALF]
            packed[step, slot, 0, i] = jnp.where(top_half, a, swap_halves(b))
            packed[step, slot, 1, i] = jnp.where(top_half, swap_halves(a), b)
            return 0

        lax.fori_loop(0, HALF, row, 0, unroll=True)

        @pl.when(v > 0)
        def _():
            mix_copy(step, slot, -1).start()

        @pl.when(v < 3)
        def _():
            mix_copy(step, slot, 1).start()

    def mix_wait(step, slot):
        @pl.when(v > 0)
        def _():
            mix_copy(step, slot, 1).wait_recv()

        @pl.when(v < 3)
        def _():
            mix_copy(step, slot, -1).wait_recv()

    def mix_sent(step, slot):
        @pl.when(v > 0)
        def _():
            mix_copy(step, slot, -1).wait_send()

        @pl.when(v < 3)
        def _():
            mix_copy(step, slot, 1).wait_send()

    def settle(step, put, start, stop):
        def reacted(i, beyond_of):
            inner = mix_w[i, 0]
            outer = mix_w[i, 1]
            mixed = []
            for slot in range(4):
                a = second[slot, i]
                beyond = beyond_of(slot)
                mixed.append(a + inner * (swap_halves(a) - a) + outer * (beyond - a))
            whole = jnp.concatenate(mixed, axis=0)
            soft = whole / (1.0 + jnp.abs(whole))
            done = whole + jnp.dot(
                matrix[...], soft, precision=lax.Precision.HIGHEST, preferred_element_type=F32
            )
            for slot in range(4):
                put(slot, i, done[8 * slot : 8 * slot + 8])

        def rows(j, _):
            reacted(
                j,
                lambda slot: jnp.where(
                    top_half, ext[step, 0, slot, j], swap_halves(ext[step, 1, slot, j])
                ),
            )
            reacted(
                j + HALF,
                lambda slot: jnp.where(
                    top_half, swap_halves(ext[step, 0, slot, j]), ext[step, 1, slot, j]
                ),
            )
            return 0

        lax.fori_loop(start, stop, rows, 0)

    order = [w, 2 * (1 - c) + t, 2 * c + 1 - t, 2 * (1 - c) + 1 - t]

    between = jnp.logical_or(
        jnp.logical_and(has_prev, odd(sp - 1) != flip),
        jnp.logical_and(has_next, odd(sp + 1) != flip),
    )

    def run(step):
        if step == 0:

            @pl.when(between)
            def _():
                for number in range(2):
                    arrived(number)

        for number, slot in enumerate(order):
            halo_wait(step, slot)
            advance(step, slot)
            mix_start(step, slot)
            if step == 0 and number < 2:

                @pl.when(jnp.logical_not(between))
                def _(number=number):
                    arrived(number)
        for slot in order:
            mix_wait(step, slot)

    run(0)

    def put_next(slot, i, a):
        grid[1, slot, GHOST + i] = a

    settle(0, put_next, 0, HALF)
    for slot in order:
        halo_start(1, slot)
    run(1)

    def put_final(slot, i, a):
        final[slot, i] = a

    cuts = [(h, HALF * side + 2 * h) for h in range(2) for side in range(2)]

    def out_copy(k, part_of, row):
        cc, tt = peers[k]
        return remote(
            final.at[2 * cc + tt, pl.ds(row, 2)], out.at[v, pl.ds(row, 2)],
            out_s.at[k, part_of], out_r.at[v, part_of], at(cc, sp, tt),
        )

    def own_copy(part_of, row):
        return pltpu.make_async_copy(
            final.at[w, pl.ds(row, 2)], out.at[v, pl.ds(row, 2)], own_out.at[part_of]
        )

    for h in range(2):
        settle(1, put_final, 2 * h, 2 * h + 2)
        for part_of, (when, row) in enumerate(cuts):
            if when == h:
                for k in range(3):
                    out_copy(k, part_of, row).start()
                own_copy(part_of, row).start()

    for part_of, (_, row) in enumerate(cuts):
        own_copy(part_of, row).wait()

    @pl.when(flip == 0)
    def _():
        velocity_own.wait()
        velocity_copy(1 - c).wait_send()
        velocity_from(1 - c).wait_recv()
        flow_copy(1 - c).wait_send()

    @pl.when(flip == 1)
    def _():
        for cc in range(2):
            velocity_copy(cc).wait_send()
            velocity_from(cc).wait_recv()
            flow_copy(cc).wait_send()

    for k in range(3):
        for e in range(2):
            in_copy(k, e).wait_send()

    @pl.when(has_prev)
    def _():
        dep_copy(-1).wait_send()
        relay_copy(-1).wait_send()

    @pl.when(has_next)
    def _():
        dep_copy(1).wait_send()
        relay_copy(1).wait_send()

    for step in range(STEPS):
        for slot in range(4):
            halo_sent(step, slot)
            mix_sent(step, slot)
    for k in range(3):
        cc, tt = peers[k]
        source = pair_of(cc, tt)
        for part_of, (_, row) in enumerate(cuts):
            out_copy(k, part_of, row).wait_send()
            remote(
                final.at[w, pl.ds(row, 2)], out.at[source, pl.ds(row, 2)],
                out_s.at[k, part_of], out_r.at[source, part_of], at(cc, sp, tt),
            ).wait_recv()


def place(blocks, flow, out, flow_out, held, held_flow, ready, sems):
    ny = blocks.shape[-1]
    loads = [pltpu.make_async_copy(blocks.at[g], held.at[g], sems.at[5 + g]) for g in range(4)]
    for load in loads:
        load.start()
    flow_in = pltpu.make_async_copy(flow, held_flow, sems.at[9])
    flow_in.start()
    copies = []
    for pair in range(4):
        loads[pair].wait()

        def tile(q, _):
            lanes = pl.ds(pl.multiple_of(q * 128, 128), 128)
            x = jnp.swapaxes(held[pair, :, :, lanes], 0, 1)
            for e in range(2):
                for s in range(4):
                    ready[pair, s, e, :, lanes] = x[4 * e + s]
            return 0

        lax.fori_loop(0, ny // 128, tile, 0, unroll=4)
        copy = pltpu.make_async_copy(ready.at[pair], out.at[:, pl.ds(2 * pair, 2)], sems.at[pair])
        copy.start()
        copies.append(copy)
    flow_in.wait()
    flow_copy = pltpu.make_async_copy(held_flow, flow_out, sems.at[4])
    flow_copy.start()
    for copy in copies:
        copy.wait()
    flow_copy.wait()


def body(tracers, flow, reaction_rates, land_mask, layers):
    ny = tracers.shape[-1]
    vmem = pl.BlockSpec(memory_space=pltpu.VMEM)
    anywhere = pl.BlockSpec(memory_space=pl.ANY)
    dma = pltpu.SemaphoreType.DMA
    blocks, flow_done = pl.pallas_call(
        kernel,
        out_shape=(
            jax.ShapeDtypeStruct((4, ROWS, 8, ny), F32),
            jax.ShapeDtypeStruct((4, ROWS, ny), F32),
        ),
        in_specs=[pl.BlockSpec(memory_space=pltpu.HBM)] * 2 + [vmem] * 3,
        out_specs=(anywhere, anywhere),
        scratch_shapes=[
            pltpu.VMEM((4, 8, ROWS, ny), F32),
            pltpu.VMEM((4, ROWS, ny), F32),
            pltpu.VMEM((ROWS, ny), F32),
            pltpu.VMEM((32, 32), F32),
            pltpu.VMEM((4, 2, 4, ROWS, ny), F32),
            pltpu.VMEM((STEPS, 4, SPAN, 8, ny), F32),
            pltpu.VMEM((SPAN, 8, ny), F32),
            pltpu.VMEM((SPAN, 8, ny), F32),
            pltpu.VMEM((4, ROWS, 8, ny), F32),
            pltpu.VMEM((STEPS, 13, 4, 8, ny), F32),
            pltpu.VMEM((STEPS, 12, 4, 8, ny), F32),
            pltpu.VMEM((ROWS, 2, 8, ny), F32),
            pltpu.VMEM((2, 8, DEEP, ny), F32),
            pltpu.VMEM((STEPS + 1, 2, 2, DEEP, ny), F32),
            pltpu.VMEM((DEEP, ny), F32),
            pltpu.VMEM((STEPS, 4, 2, HALF, 8, ny), F32),
            pltpu.VMEM((STEPS, 2, 4, HALF, 8, ny), F32),
            pltpu.VMEM((4, ROWS, 8, ny), F32),
            pltpu.VMEM((2, 2, ROWS, ny), F32),
            dma((3,)), dma((3, 2)), dma((4, 2)),
            dma((2,)), dma((2,)), dma((2,)), dma((3,)), dma((3,)), dma((3,)), dma((3,)),
            dma((STEPS, 4, 2)), dma((STEPS, 4, 2)),
            dma((STEPS, 4, 2)), dma((STEPS, 4, 2)),
            dma((3, 4)), dma((4, 4)), dma((4,)),
            dma((2,)), dma((2,)), dma((1,)),
        ],
        compiler_params=pltpu.CompilerParams(
            collective_id=0, has_side_effects=True, vmem_limit_bytes=ALL_VMEM
        ),
        name="ocean",
    )(tracers, flow, reaction_rates, land_mask, layers)
    return pl.pallas_call(
        place,
        out_shape=(
            jax.ShapeDtypeStruct(tracers.shape, F32),
            jax.ShapeDtypeStruct(flow.shape, F32),
        ),
        in_specs=[pl.BlockSpec(memory_space=pltpu.HBM)] * 2,
        out_specs=(pl.BlockSpec(memory_space=pltpu.HBM),) * 2,
        scratch_shapes=[
            pltpu.VMEM((4, ROWS, 8, ny), F32),
            pltpu.VMEM((4, ROWS, ny), F32),
            pltpu.VMEM((4, 4, 2, ROWS, ny), F32),
            dma((10,)),
        ],
        compiler_params=pltpu.CompilerParams(vmem_limit_bytes=ALL_VMEM),
        name="place",
    )(blocks, flow_done)


def solution(mesh):
    placed = (
        P(("comp", "trc"), None, "space", None),
        P(("comp", "trc"), "space", None),
        P(),
        P("space", None),
        P("space", None),
    )
    return jax.shard_map(
        body,
        mesh=mesh,
        in_specs=placed,
        out_specs=(P(("comp", "trc"), None, "space", None), P(("comp", "trc"), "space", None)),
        check_vma=False,
    )
```

```python
import functools

import jax
import jax.numpy as jnp
from jax import lax
from jax.experimental import pallas as pl
from jax.experimental.pallas import tpu as pltpu
from jax.sharding import PartitionSpec as P

STEPS = 2
COURANT = 0.25
VISCOSITY = 0.2
CORIOLIS = 0.3
FRICTION = 0.1
DIFFUSION = 0.3
REACT_STEP = 0.5

MESH = pl.DeviceIdType.MESH
F32 = jnp.float32
ROWS = 8
DEEP = 24
GHOST = 4
SPAN = ROWS + 2 * GHOST
EDGE = 128
HALF = ROWS // 2
ALL_VMEM = 67_043_328
LINE = 8
PAIR = 128
PAIRS = 2


def limited(before, after):
    return jnp.maximum(jnp.minimum(after, 0.0), jnp.minimum(before, jnp.maximum(after, 0.0)))


def roll_lanes(a, by):
    return pltpu.roll(a, by % a.shape[-1], a.ndim - 1)


def kernel(
    tracers, flow, rates, land, layers, out, flow_out,
    tr_v, fl_v, dep_v, matrix, stage, grid, first, part, second, coef_x, coef_y, mix_w, natural,
    field, depth_v, packed, ext, final, velocity_send,
    in_local, in_sem_s, in_sem_r, fl_local, fl_sem_s, fl_sem_r, rel_s, rel_r, dep_s, dep_r,
    halo_s, halo_r, mix_s, mix_r, out_s, out_r, own_out, fo_s, fo_r, fo_own,
):
    ny = tracers.shape[-1]
    c = lax.axis_index("comp")
    sp = lax.axis_index("space")
    t = lax.axis_index("trc")
    n = lax.axis_size("space")
    w = 2 * c + t
    has_prev = sp > 0
    has_next = sp < n - 1

    def odd(strip):
        return lax.rem(strip // LINE, 2)

    def flipped(bit, strip):
        return lax.rem(bit + odd(strip), 2)

    flip = odd(sp)
    tl = flipped(t, sp)
    v = 2 * tl + c

    def at(cc, ss, tt):
        return {"comp": cc, "space": ss, "trc": tt}

    def holder(pair, strip):
        return at(lax.rem(pair, 2), strip, flipped(pair // 2, strip))

    def remote(src, dst, s, r, dev):
        return pltpu.make_async_remote_copy(
            src_ref=src, dst_ref=dst, send_sem=s, recv_sem=r, device_id=dev, device_id_type=MESH
        )

    middle = pl.ds(ROWS, ROWS)
    mid = ny // 2
    cut = mid + EDGE
    width = mid + EDGE

    all_flow = pltpu.make_async_copy(flow, fl_v, fl_local.at[1])
    all_tr = pltpu.make_async_copy(tracers, tr_v, in_local.at[0])
    own_tr = [
        pltpu.make_async_copy(tracers.at[:, 2 * v + e], stage.at[w, e], in_local.at[1 + e])
        for e in range(2)
    ]
    my_flow = pltpu.make_async_copy(
        flow.at[pl.ds(2 * c, 2)], field.at[0, c, :, middle], fl_local.at[0]
    )
    all_flow.start()
    all_tr.start()
    for copy in own_tr:
        copy.start()

    @pl.when(flip == 0)
    def _():
        my_flow.start()

    barrier = pltpu.get_barrier_semaphore()
    peers = [(c, 1 - t), (1 - c, 1 - t), (1 - c, t)]

    def pair_of(cc, tt):
        return 2 * flipped(tt, sp) + cc

    for cc, tt in peers:
        pl.semaphore_signal(barrier, inc=1, device_id=at(cc, sp, tt), device_id_type=MESH)

    @pl.when(has_prev)
    def _():
        pl.semaphore_signal(barrier, inc=1, device_id=holder(v, sp - 1), device_id_type=MESH)

    @pl.when(has_next)
    def _():
        pl.semaphore_signal(barrier, inc=1, device_id=holder(v, sp + 1), device_id_type=MESH)

    dep_v[...] = jnp.where(land[...] > 0, layers[...], 0).astype(F32)
    depth_v[middle] = dep_v[...]

    @pl.when(jnp.logical_not(has_prev))
    def _():
        depth_v[0:ROWS] = jnp.zeros((ROWS, ny), F32)
        for comp in range(2):
            for e in range(2):
                field[0, comp, e, 0:ROWS] = jnp.zeros((ROWS, ny), F32)
        for step in range(2):
            for slot in range(4):
                for row in range(GHOST):
                    grid[step, slot, row] = jnp.zeros((8, ny), F32)

    @pl.when(jnp.logical_not(has_next))
    def _():
        depth_v[2 * ROWS :] = jnp.zeros((ROWS, ny), F32)
        for comp in range(2):
            for e in range(2):
                field[0, comp, e, 2 * ROWS :] = jnp.zeros((ROWS, ny), F32)
        for step in range(2):
            for slot in range(4):
                for row in range(GHOST):
                    grid[step, slot, GHOST + ROWS + row] = jnp.zeros((8, ny), F32)

    @pl.when(v == 0)
    def _():
        for step in range(2):
            for slot in range(4):
                ext[step, 0, slot] = jnp.zeros((HALF, 8, ny), F32)

    @pl.when(v == 3)
    def _():
        for step in range(2):
            for slot in range(4):
                ext[step, 1, slot] = jnp.zeros((HALF, 8, ny), F32)

    lines = lax.broadcasted_iota(jnp.int32, (32, 16), 0)
    names = lax.broadcasted_iota(jnp.int32, (32, 16), 1)
    pick = jnp.where(4 * (lines // 8) + lax.rem(lines, 4) == names, 1.0, 0.0)
    wide = jnp.dot(pick, rates[...], precision=lax.Precision.HIGHEST, preferred_element_type=F32)
    wide = lax.dot_general(
        wide, pick, (((1,), (1,)), ((), ())),
        precision=lax.Precision.HIGHEST, preferred_element_type=F32,
    )
    line = lax.broadcasted_iota(jnp.int32, (32, 32), 0)
    other = lax.broadcasted_iota(jnp.int32, (32, 32), 1)
    same_level = lax.rem(line // 4, 2) == lax.rem(other // 4, 2)
    matrix[...] = jnp.where(same_level, REACT_STEP * wide, 0.0)

    all_flow.wait()
    pl.semaphore_wait(barrier, 3 + jnp.where(has_prev, 1, 0) + jnp.where(has_next, 1, 0))

    def flow_copy(cc):
        return remote(
            fl_v.at[pl.ds(2 * cc, 2)], field.at[0, c, :, middle],
            fl_sem_s.at[cc], fl_sem_r.at[c], holder(2 * t + cc, sp),
        )

    def flow_from(cc):
        return remote(
            fl_v.at[pl.ds(0, 2)], field.at[0, cc, :, middle],
            fl_sem_s.at[cc], fl_sem_r.at[cc], at(cc, sp, tl),
        )

    @pl.when(flip == 0)
    def _():
        flow_copy(1 - c).start()

    @pl.when(flip == 1)
    def _():
        for cc in range(2):
            flow_copy(cc).start()

    def in_copy(k, e):
        cc, tt = peers[k]
        return remote(
            tr_v.at[:, 2 * pair_of(cc, tt) + e], stage.at[w, e],
            in_sem_s.at[k, e], in_sem_r.at[w, e], at(cc, sp, tt),
        )

    all_tr.wait()
    for k in (2, 0, 1):
        for e in range(2):
            in_copy(k, e).start()

    def dep_copy(d):
        return remote(
            dep_v, depth_v.at[pl.ds(ROWS * (1 - d), ROWS)],
            dep_s.at[d + 1], dep_r.at[1 - d], holder(v, sp + d),
        )

    def relay_copy(d):
        return remote(
            field.at[0, :, :, middle], field.at[0, :, :, pl.ds(ROWS * (1 - d), ROWS)],
            rel_s.at[d + 1], rel_r.at[1 - d], holder(v, sp + d),
        )

    @pl.when(has_prev)
    def _():
        dep_copy(-1).start()

    @pl.when(has_next)
    def _():
        dep_copy(1).start()

    def halo_copy(wave, slot, d):
        low = d < 0
        step, lanes = ((0, pl.ds(0, ny)), (1, pl.ds(0, cut)), (1, pl.ds(cut, ny - cut)))[wave]
        return remote(
            grid.at[step, slot, pl.ds(GHOST if low else ROWS, GHOST), :, lanes],
            grid.at[step, slot, pl.ds(GHOST + ROWS if low else 0, GHOST), :, lanes],
            halo_s.at[wave, slot, 0 if low else 1], halo_r.at[wave, slot, 1 if low else 0],
            holder(v, sp + d),
        )

    def halo_start(wave, slot):
        @pl.when(has_prev)
        def _():
            halo_copy(wave, slot, -1).start()

        @pl.when(has_next)
        def _():
            halo_copy(wave, slot, 1).start()

    def halo_wait(wave, slot):
        @pl.when(has_prev)
        def _():
            halo_copy(wave, slot, 1).wait_recv()

        @pl.when(has_next)
        def _():
            halo_copy(wave, slot, -1).wait_recv()

    def halo_sent(wave, slot):
        @pl.when(has_prev)
        def _():
            halo_copy(wave, slot, -1).wait_send()

        @pl.when(has_next)
        def _():
            halo_copy(wave, slot, 1).wait_send()

    def regroup(slot):
        def tile(q, _):
            lanes = pl.ds(pl.multiple_of(q * 128, 128), 128)
            x = stage[slot, :, :, :, lanes].reshape(8, ROWS, 128)
            grid[0, slot, pl.ds(GHOST, ROWS), :, lanes] = jnp.swapaxes(x, 0, 1)
            return 0

        lax.fori_loop(0, ny // 128, tile, 0, unroll=2)

    def arrived(k):
        cc, tt = peers[k]
        slot = 2 * cc + tt
        for e in range(2):
            remote(
                stage.at[slot, e], stage.at[slot, e], in_sem_s.at[k, e], in_sem_r.at[slot, e],
                at(cc, sp, tt),
            ).wait_recv()
        regroup(slot)
        halo_start(0, slot)

    for copy in own_tr:
        copy.wait()
    regroup(w)

    @pl.when(flip == 0)
    def _():
        my_flow.wait()
        flow_from(1 - c).wait_recv()

    @pl.when(flip == 1)
    def _():
        for cc in range(2):
            flow_from(cc).wait_recv()

    @pl.when(has_prev)
    def _():
        relay_copy(-1).start()

    @pl.when(has_next)
    def _():
        relay_copy(1).start()

    halo_start(0, w)
    arrived(2)

    @pl.when(has_prev)
    def _():
        dep_copy(1).wait_recv()
        relay_copy(1).wait_recv()

    @pl.when(has_next)
    def _():
        dep_copy(-1).wait_recv()
        relay_copy(-1).wait_recv()

    lane_deep = lax.broadcasted_iota(jnp.int32, (DEEP, ny), 1)
    top_half = lax.broadcasted_iota(jnp.int32, (8, ny), 0) < 4

    def wet_of(level, rows):
        return jnp.where(depth_v[rows] > level.astype(F32), 1.0, 0.0)

    def lap(a):
        left = jnp.where(lane_deep == 0, 0.0, roll_lanes(a, 1))
        right = jnp.where(lane_deep == ny - 1, 0.0, roll_lanes(a, -1))
        return pltpu.roll(a, 1, 0) + pltpu.roll(a, DEEP - 1, 0) + left + right - 4.0 * a

    def put_coefs(e, base, face):
        up = jnp.maximum(face, 0.0)
        down = jnp.minimum(face, 0.0)
        natural[e, base] = -COURANT * up
        natural[e, base + 1] = (-COURANT * 0.5) * up * (1.0 - COURANT * up)
        natural[e, base + 2] = -COURANT * down
        natural[e, base + 3] = (COURANT * 0.5) * down * (1.0 + COURANT * down)

    def spread_rows(ref, k, j):
        one = jnp.broadcast_to(ref[0, k, j : j + 1, :], (8, ny))
        two = jnp.broadcast_to(ref[1, k, j : j + 1, :], (8, ny))
        return jnp.where(top_half, one, two)

    def velocities(step, _):
        def level(e, _):
            wet = wet_of(2 * v + e, slice(None))
            u = field[step, 0, e]
            r = field[step, 1, e]
            u_new = wet * (u + CORIOLIS * r + VISCOSITY * lap(u) - FRICTION * u)
            r_new = wet * (r - CORIOLIS * u + VISCOSITY * lap(r) - FRICTION * r)
            field[step + 1, 0, e] = u_new
            field[step + 1, 1, e] = r_new
            face = 0.5 * (u_new + pltpu.roll(u_new, DEEP - 1, 0)) * wet * pltpu.roll(wet, DEEP - 1, 0)
            put_coefs(e, 0, face)
            wet_right = jnp.where(lane_deep == ny - 1, 0.0, roll_lanes(wet, -1))
            face = 0.5 * (r_new + roll_lanes(r_new, -1)) * wet * wet_right
            put_coefs(e, 4, face)
            return 0

        lax.fori_loop(0, 2, level, 0)
        shift = ROWS - GHOST
        for i in range(1, 14):
            for k in range(4):
                coef_x[step, i - 1, k] = spread_rows(natural, k, i + shift)
        for i in range(2, 14):
            for k in range(4):
                coef_y[step, i - 2, k] = spread_rows(natural, 4 + k, i + shift)
        return 0

    velocities(0, 0)

    def velocity_copy(comp):
        return remote(
            velocity_send.at[comp], flow_out.at[pl.ds(2 * c, 2)],
            fo_s.at[comp], fo_r.at[c], at(comp, sp, tl),
        )

    def velocity_from(cc):
        return remote(
            velocity_send.at[0], flow_out.at[pl.ds(2 * cc, 2)],
            fo_s.at[0], fo_r.at[cc], holder(2 * t + cc, sp),
        )

    velocity_own = pltpu.make_async_copy(
        velocity_send.at[c], flow_out.at[pl.ds(2 * c, 2)], fo_own.at[0]
    )

    def later_velocities():
        velocities(1, 0)
        own_rows = slice(ROWS, 2 * ROWS)
        above = jnp.where(v > 0, DIFFUSION, 0.0).astype(F32)
        wet_a = wet_of(2 * v, own_rows)
        wet_b = wet_of(2 * v + 1, own_rows)
        natural[0, 0, 0:ROWS] = DIFFUSION * wet_a * wet_b
        natural[1, 0, 0:ROWS] = DIFFUSION * wet_a * wet_b
        natural[0, 1, 0:ROWS] = above * wet_a * wet_of(2 * v - 1, own_rows)
        natural[1, 1, 0:ROWS] = DIFFUSION * wet_b * wet_of(2 * v + 2, own_rows)
        for row in range(ROWS):
            for k in range(2):
                mix_w[row, k] = spread_rows(natural, k, row)

        for comp in range(2):
            for e in range(2):
                velocity_send[comp, e] = field[STEPS, comp, e, own_rows]

        @pl.when(flip == 0)
        def _():
            velocity_own.start()
            velocity_copy(1 - c).start()

        @pl.when(flip == 1)
        def _():
            for comp in range(2):
                velocity_copy(comp).start()

    def along_x(step, load, first_face, last_face, start, size, put):
        def chunk(q, _):
            lanes = pl.ds(pl.multiple_of(start + q * PAIR, 128), PAIR)
            before = load(first_face - 1, lanes)
            here = load(first_face, lanes)
            ahead = load(first_face + 1, lanes)
            jump = ahead - here
            slope = limited(here - before, jump)
            last_flux = None
            for i in range(first_face, last_face + 1):
                far = load(i + 2, lanes)
                next_jump = far - ahead
                next_slope = limited(jump, next_jump)
                k = i - 1
                flux = (
                    coef_x[step, k, 0, :, lanes] * here
                    + coef_x[step, k, 1, :, lanes] * slope
                    + coef_x[step, k, 2, :, lanes] * ahead
                    + coef_x[step, k, 3, :, lanes] * next_slope
                )
                if last_flux is not None:
                    put(i, lanes, here, flux - last_flux)
                last_flux = flux
                here, ahead, jump, slope = ahead, far, next_jump, next_slope
            return 0

        lax.fori_loop(0, size // PAIR, chunk, 0, unroll=PAIRS)

    def along_y(step, i, a, lanes):
        columns = lax.broadcasted_iota(jnp.int32, a.shape, 1)
        right = jnp.where(columns == a.shape[1] - 1, 0.0, roll_lanes(a, -1))
        jump = right - a
        slope = limited(jnp.where(columns == 0, a, roll_lanes(jump, 1)), jump)
        flux = (
            coef_y[step, i - 2, 0, :, lanes] * a
            + coef_y[step, i - 2, 1, :, lanes] * slope
            + coef_y[step, i - 2, 2, :, lanes] * right
            + coef_y[step, i - 2, 3, :, lanes] * roll_lanes(slope, -1)
        )
        return flux - jnp.where(columns == 0, 0.0, roll_lanes(flux, 1))

    def advance(step, slot, start, size, keep_start, keep_size):
        lanes = pl.ds(start, size)
        kept = pl.ds(keep_start, keep_size)
        skip = keep_start - start

        def put_one(i, at_lanes, here, change):
            part[i, :, at_lanes] = here + change

        along_x(
            step, lambda i, at_lanes: grid[step, slot, i, :, at_lanes], 1, 13, start, size, put_one
        )

        def row_one(i, _):
            first[i, :, lanes] = part[i, :, lanes] + along_y(
                step, i, grid[step, slot, i, :, lanes], lanes
            )
            return 0

        lax.fori_loop(2, 14, row_one, 0, unroll=True)

        def put_two(i, at_lanes, here, change):
            part[i, :, at_lanes] = (grid[step, slot, i, :, at_lanes] + here) + change

        along_x(
            step, lambda i, at_lanes: first[i, :, at_lanes], 3, 11, keep_start, keep_size, put_two
        )

        def row_two(i, _):
            change = along_y(step, i, first[i, :, lanes], lanes)
            second[slot, i - GHOST, :, kept] = 0.5 * (
                part[i, :, kept] + change[:, skip : skip + keep_size]
            )
            return 0

        lax.fori_loop(GHOST, GHOST + ROWS, row_two, 0, unroll=True)

    def swap_halves(a):
        return pltpu.roll(a, 4, 0)

    kept_of = ((0, ny), (0, mid), (mid, ny - mid))

    def mix_copy(wave, slot, d):
        step, lanes = min(wave, 1), pl.ds(*kept_of[wave])
        return remote(
            packed.at[step, slot, 0 if d < 0 else 1, :, :, lanes],
            ext.at[step, 1 if d < 0 else 0, slot, :, :, lanes],
            mix_s.at[wave, slot, 0 if d < 0 else 1], mix_r.at[wave, slot, 1 if d < 0 else 0],
            holder(v + d, sp),
        )

    def mix_start(wave, slot):
        step, lanes = min(wave, 1), pl.ds(*kept_of[wave])
        in_top = lax.broadcasted_iota(jnp.int32, (8, kept_of[wave][1]), 0) < 4

        def row(i, _):
            a = second[slot, i, :, lanes]
            b = second[slot, i + HALF, :, lanes]
            packed[step, slot, 0, i, :, lanes] = jnp.where(in_top, a, swap_halves(b))
            packed[step, slot, 1, i, :, lanes] = jnp.where(in_top, swap_halves(a), b)
            return 0

        lax.fori_loop(0, HALF, row, 0, unroll=True)

        @pl.when(v > 0)
        def _():
            mix_copy(wave, slot, -1).start()

        @pl.when(v < 3)
        def _():
            mix_copy(wave, slot, 1).start()

    def mix_wait(wave, slot):
        @pl.when(v > 0)
        def _():
            mix_copy(wave, slot, 1).wait_recv()

        @pl.when(v < 3)
        def _():
            mix_copy(wave, slot, -1).wait_recv()

    def mix_sent(wave, slot):
        @pl.when(v > 0)
        def _():
            mix_copy(wave, slot, -1).wait_send()

        @pl.when(v < 3)
        def _():
            mix_copy(wave, slot, 1).wait_send()

    def settle(step, put, start, size):
        lanes = pl.ds(start, size)
        in_top = lax.broadcasted_iota(jnp.int32, (8, size), 0) < 4

        def reacted(i, beyond_of):
            inner = mix_w[i, 0, :, lanes]
            outer = mix_w[i, 1, :, lanes]
            mixed = []
            for slot in range(4):
                a = second[slot, i, :, lanes]
                beyond = beyond_of(slot)
                mixed.append(a + inner * (swap_halves(a) - a) + outer * (beyond - a))
            whole = jnp.concatenate(mixed, axis=0)
            soft = whole / (1.0 + jnp.abs(whole))
            done = whole + jnp.dot(
                matrix[...], soft, precision=lax.Precision.HIGHEST, preferred_element_type=F32
            )
            for slot in range(4):
                put(slot, i, lanes, done[8 * slot : 8 * slot + 8])

        def rows(j, _):
            reacted(
                j,
                lambda slot: jnp.where(
                    in_top,
                    ext[step, 0, slot, j, :, lanes],
                    swap_halves(ext[step, 1, slot, j, :, lanes]),
                ),
            )
            reacted(
                j + HALF,
                lambda slot: jnp.where(
                    in_top,
                    swap_halves(ext[step, 0, slot, j, :, lanes]),
                    ext[step, 1, slot, j, :, lanes],
                ),
            )
            return 0

        lax.fori_loop(0, HALF, rows, 0)

    between = jnp.logical_or(
        jnp.logical_and(has_prev, odd(sp - 1) != flip),
        jnp.logical_and(has_next, odd(sp + 1) != flip),
    )
    near, far, last = 2 * (1 - c) + t, 2 * c + 1 - t, 2 * (1 - c) + 1 - t
    order = [
        w, jnp.where(between, far, near), jnp.where(between, last, far),
        jnp.where(between, near, last),
    ]

    arrived(0)
    for number, slot in enumerate(order):
        if number == 2:
            arrived(1)
        if number == 3:
            later_velocities()
        halo_wait(0, slot)
        advance(0, slot, 0, ny, 0, ny)
        mix_start(0, slot)
    for slot in range(4):
        mix_wait(0, slot)

    def put_next(slot, i, lanes, a):
        grid[1, slot, GHOST + i, :, lanes] = a

    for wave, (start, size) in ((1, (0, cut)), (2, (cut, ny - cut))):
        settle(0, put_next, start, size)
        for slot in range(4):
            halo_start(wave, slot)

    def put_final(slot, i, lanes, a):
        final[slot, i, :, lanes] = a

    def out_copy(k, wave):
        cc, tt = peers[k]
        lanes = pl.ds(*kept_of[wave])
        return remote(
            final.at[2 * cc + tt, :, :, lanes], out.at[v, :, :, lanes],
            out_s.at[k, wave], out_r.at[v, wave], at(cc, sp, tt),
        )

    def out_from(k, wave):
        cc, tt = peers[k]
        lanes = pl.ds(*kept_of[wave])
        source = pair_of(cc, tt)
        return remote(
            final.at[w, :, :, lanes], out.at[source, :, :, lanes],
            out_s.at[k, wave], out_r.at[source, wave], at(cc, sp, tt),
        )

    def own_copy(wave):
        lanes = pl.ds(*kept_of[wave])
        return pltpu.make_async_copy(
            final.at[w, :, :, lanes], out.at[v, :, :, lanes], own_out.at[wave]
        )

    def window(wave, slots):
        def one(slot, _):
            halo_wait(wave, slot)
            start = (0, ny - width)[wave - 1]
            advance(1, slot, start, width, *kept_of[wave])
            mix_start(wave, slot)
            return 0

        lax.fori_loop(*slots, one, 0)

    def finish(wave):
        for slot in range(4):
            mix_wait(wave, slot)
        settle(1, put_final, *kept_of[wave])
        for k in range(3):
            out_copy(k, wave).start()
        own_copy(wave).start()

    window(1, (0, 4))
    window(2, (0, 2))
    finish(1)
    window(2, (2, 4))
    finish(2)

    for wave in (1, 2):
        own_copy(wave).wait()

    @pl.when(flip == 0)
    def _():
        velocity_own.wait()
        velocity_copy(1 - c).wait_send()
        velocity_from(1 - c).wait_recv()
        flow_copy(1 - c).wait_send()

    @pl.when(flip == 1)
    def _():
        for cc in range(2):
            velocity_copy(cc).wait_send()
            velocity_from(cc).wait_recv()
            flow_copy(cc).wait_send()

    for k in range(3):
        for e in range(2):
            in_copy(k, e).wait_send()

    @pl.when(has_prev)
    def _():
        dep_copy(-1).wait_send()
        relay_copy(-1).wait_send()

    @pl.when(has_next)
    def _():
        dep_copy(1).wait_send()
        relay_copy(1).wait_send()

    for wave in range(3):
        for slot in range(4):
            halo_sent(wave, slot)
            mix_sent(wave, slot)
    for wave in (1, 2):
        for k in range(3):
            out_copy(k, wave).wait_send()
            out_from(k, wave).wait_recv()


def place(blocks, flow, out, flow_out, held, held_flow, ready, sems):
    ny = blocks.shape[-1]
    loads = [pltpu.make_async_copy(blocks.at[g], held.at[g], sems.at[5 + g]) for g in range(4)]
    for load in loads:
        load.start()
    flow_in = pltpu.make_async_copy(flow, held_flow, sems.at[9])
    flow_in.start()
    copies = []
    for pair in range(4):
        loads[pair].wait()

        def tile(q, _):
            lanes = pl.ds(pl.multiple_of(q * 128, 128), 128)
            x = jnp.swapaxes(held[pair, :, :, lanes], 0, 1)
            for e in range(2):
                for s in range(4):
                    ready[pair, s, e, :, lanes] = x[4 * e + s]
            return 0

        lax.fori_loop(0, ny // 128, tile, 0, unroll=4)
        copy = pltpu.make_async_copy(ready.at[pair], out.at[:, pl.ds(2 * pair, 2)], sems.at[pair])
        copy.start()
        copies.append(copy)
    flow_in.wait()
    flow_copy = pltpu.make_async_copy(held_flow, flow_out, sems.at[4])
    flow_copy.start()
    for copy in copies:
        copy.wait()
    flow_copy.wait()


def body(tracers, flow, reaction_rates, land_mask, layers):
    ny = tracers.shape[-1]
    vmem = pl.BlockSpec(memory_space=pltpu.VMEM)
    anywhere = pl.BlockSpec(memory_space=pl.ANY)
    dma = pltpu.SemaphoreType.DMA
    blocks, flow_done = pl.pallas_call(
        kernel,
        out_shape=(
            jax.ShapeDtypeStruct((4, ROWS, 8, ny), F32),
            jax.ShapeDtypeStruct((4, ROWS, ny), F32),
        ),
        in_specs=[pl.BlockSpec(memory_space=pltpu.HBM)] * 2 + [vmem] * 3,
        out_specs=(anywhere, anywhere),
        scratch_shapes=[
            pltpu.VMEM((4, 8, ROWS, ny), F32),
            pltpu.VMEM((4, ROWS, ny), F32),
            pltpu.VMEM((ROWS, ny), F32),
            pltpu.VMEM((32, 32), F32),
            pltpu.VMEM((4, 2, 4, ROWS, ny), F32),
            pltpu.VMEM((STEPS, 4, SPAN, 8, ny), F32),
            pltpu.VMEM((SPAN, 8, ny), F32),
            pltpu.VMEM((SPAN, 8, ny), F32),
            pltpu.VMEM((4, ROWS, 8, ny), F32),
            pltpu.VMEM((STEPS, 13, 4, 8, ny), F32),
            pltpu.VMEM((STEPS, 12, 4, 8, ny), F32),
            pltpu.VMEM((ROWS, 2, 8, ny), F32),
            pltpu.VMEM((2, 8, DEEP, ny), F32),
            pltpu.VMEM((STEPS + 1, 2, 2, DEEP, ny), F32),
            pltpu.VMEM((DEEP, ny), F32),
            pltpu.VMEM((STEPS, 4, 2, HALF, 8, ny), F32),
            pltpu.VMEM((STEPS, 2, 4, HALF, 8, ny), F32),
            pltpu.VMEM((4, ROWS, 8, ny), F32),
            pltpu.VMEM((2, 2, ROWS, ny), F32),
            dma((3,)), dma((3, 2)), dma((4, 2)),
            dma((2,)), dma((2,)), dma((2,)), dma((3,)), dma((3,)), dma((3,)), dma((3,)),
            dma((3, 4, 2)), dma((3, 4, 2)),
            dma((3, 4, 2)), dma((3, 4, 2)),
            dma((3, 3)), dma((4, 3)), dma((3,)),
            dma((2,)), dma((2,)), dma((1,)),
        ],
        compiler_params=pltpu.CompilerParams(
            collective_id=0, has_side_effects=True, vmem_limit_bytes=ALL_VMEM
        ),
        name="ocean",
    )(tracers, flow, reaction_rates, land_mask, layers)
    return pl.pallas_call(
        place,
        out_shape=(
            jax.ShapeDtypeStruct(tracers.shape, F32),
            jax.ShapeDtypeStruct(flow.shape, F32),
        ),
        in_specs=[pl.BlockSpec(memory_space=pltpu.HBM)] * 2,
        out_specs=(pl.BlockSpec(memory_space=pltpu.HBM),) * 2,
        scratch_shapes=[
            pltpu.VMEM((4, ROWS, 8, ny), F32),
            pltpu.VMEM((4, ROWS, ny), F32),
            pltpu.VMEM((4, 4, 2, ROWS, ny), F32),
            dma((10,)),
        ],
        compiler_params=pltpu.CompilerParams(vmem_limit_bytes=ALL_VMEM),
        name="place",
    )(blocks, flow_done)


def solution(mesh):
    placed = (
        P(("comp", "trc"), None, "space", None),
        P(("comp", "trc"), "space", None),
        P(),
        P("space", None),
        P("space", None),
    )
    return jax.shard_map(
        body,
        mesh=mesh,
        in_specs=placed,
        out_specs=(P(("comp", "trc"), None, "space", None), P(("comp", "trc"), "space", None)),
        check_vma=False,
    )
```

```python
import functools

import jax
import jax.numpy as jnp
from jax import lax
from jax.experimental import pallas as pl
from jax.experimental.pallas import tpu as pltpu
from jax.sharding import PartitionSpec as P

STEPS = 2
COURANT = 0.25
VISCOSITY = 0.2
CORIOLIS = 0.3
FRICTION = 0.1
DIFFUSION = 0.3
REACT_STEP = 0.5

MESH = pl.DeviceIdType.MESH
F32 = jnp.float32
ROWS = 8
DEEP = 24
GHOST = 4
SPAN = ROWS + 2 * GHOST
EDGE = 128
HALF = ROWS // 2
ALL_VMEM = 67_043_328
LINE = 8
PAIR = 128
PAIRS = 2


def limited(before, after):
    return jnp.maximum(jnp.minimum(after, 0.0), jnp.minimum(before, jnp.maximum(after, 0.0)))


def roll_lanes(a, by):
    return pltpu.roll(a, by % a.shape[-1], a.ndim - 1)


def kernel(
    tracers, flow, rates, land, layers, out, flow_out,
    tr_v, fl_v, dep_v, matrix, stage, grid, first, part, second, coef_x, coef_y, mix_w, natural,
    field, depth_v, packed, ext, final, velocity_send,
    in_local, in_sem_s, in_sem_r, fl_local, fl_sem_s, fl_sem_r, rel_s, rel_r, dep_s, dep_r,
    halo_s, halo_r, mix_s, mix_r, out_s, out_r, own_out, fo_s, fo_r, fo_own,
):
    ny = tracers.shape[-1]
    c = lax.axis_index("comp")
    sp = lax.axis_index("space")
    t = lax.axis_index("trc")
    n = lax.axis_size("space")
    w = 2 * c + t
    has_prev = sp > 0
    has_next = sp < n - 1

    def odd(strip):
        return lax.rem(strip // LINE, 2)

    def flipped(bit, strip):
        return lax.rem(bit + odd(strip), 2)

    flip = odd(sp)
    tl = flipped(t, sp)
    v = 2 * tl + c

    def at(cc, ss, tt):
        return {"comp": cc, "space": ss, "trc": tt}

    def holder(pair, strip):
        return at(lax.rem(pair, 2), strip, flipped(pair // 2, strip))

    def remote(src, dst, s, r, dev):
        return pltpu.make_async_remote_copy(
            src_ref=src, dst_ref=dst, send_sem=s, recv_sem=r, device_id=dev, device_id_type=MESH
        )

    middle = pl.ds(ROWS, ROWS)
    mid = ny // 2
    cut = mid + EDGE
    width = mid + EDGE

    all_flow = pltpu.make_async_copy(flow, fl_v, fl_local.at[1])
    all_tr = pltpu.make_async_copy(tracers, tr_v, in_local.at[0])
    own_tr = [
        pltpu.make_async_copy(tracers.at[:, 2 * v + e], stage.at[w, e], in_local.at[1 + e])
        for e in range(2)
    ]
    my_flow = pltpu.make_async_copy(
        flow.at[pl.ds(2 * c, 2)], field.at[0, c, :, middle], fl_local.at[0]
    )
    all_flow.start()
    all_tr.start()
    for copy in own_tr:
        copy.start()

    @pl.when(flip == 0)
    def _():
        my_flow.start()

    barrier = pltpu.get_barrier_semaphore()
    peers = [(c, 1 - t), (1 - c, 1 - t), (1 - c, t)]

    def pair_of(cc, tt):
        return 2 * flipped(tt, sp) + cc

    for cc, tt in peers:
        pl.semaphore_signal(barrier, inc=1, device_id=at(cc, sp, tt), device_id_type=MESH)

    @pl.when(has_prev)
    def _():
        pl.semaphore_signal(barrier, inc=1, device_id=holder(v, sp - 1), device_id_type=MESH)

    @pl.when(has_next)
    def _():
        pl.semaphore_signal(barrier, inc=1, device_id=holder(v, sp + 1), device_id_type=MESH)

    dep_v[...] = jnp.where(land[...] > 0, layers[...], 0).astype(F32)
    depth_v[middle] = dep_v[...]

    @pl.when(jnp.logical_not(has_prev))
    def _():
        depth_v[0:ROWS] = jnp.zeros((ROWS, ny), F32)
        for comp in range(2):
            for e in range(2):
                field[0, comp, e, 0:ROWS] = jnp.zeros((ROWS, ny), F32)
        for step in range(2):
            for slot in range(4):
                for row in range(GHOST):
                    grid[step, slot, row] = jnp.zeros((8, ny), F32)

    @pl.when(jnp.logical_not(has_next))
    def _():
        depth_v[2 * ROWS :] = jnp.zeros((ROWS, ny), F32)
        for comp in range(2):
            for e in range(2):
                field[0, comp, e, 2 * ROWS :] = jnp.zeros((ROWS, ny), F32)
        for step in range(2):
            for slot in range(4):
                for row in range(GHOST):
                    grid[step, slot, GHOST + ROWS + row] = jnp.zeros((8, ny), F32)

    @pl.when(v == 0)
    def _():
        for step in range(2):
            for slot in range(4):
                ext[step, 0, slot] = jnp.zeros((HALF, 8, ny), F32)

    @pl.when(v == 3)
    def _():
        for step in range(2):
            for slot in range(4):
                ext[step, 1, slot] = jnp.zeros((HALF, 8, ny), F32)

    lines = lax.broadcasted_iota(jnp.int32, (32, 16), 0)
    names = lax.broadcasted_iota(jnp.int32, (32, 16), 1)
    pick = jnp.where(4 * (lines // 8) + lax.rem(lines, 4) == names, 1.0, 0.0)
    wide = jnp.dot(pick, rates[...], precision=lax.Precision.HIGHEST, preferred_element_type=F32)
    wide = lax.dot_general(
        wide, pick, (((1,), (1,)), ((), ())),
        precision=lax.Precision.HIGHEST, preferred_element_type=F32,
    )
    line = lax.broadcasted_iota(jnp.int32, (32, 32), 0)
    other = lax.broadcasted_iota(jnp.int32, (32, 32), 1)
    same_level = lax.rem(line // 4, 2) == lax.rem(other // 4, 2)
    matrix[...] = jnp.where(same_level, REACT_STEP * wide, 0.0)

    all_flow.wait()
    pl.semaphore_wait(barrier, 3 + jnp.where(has_prev, 1, 0) + jnp.where(has_next, 1, 0))

    def flow_copy(cc):
        return remote(
            fl_v.at[pl.ds(2 * cc, 2)], field.at[0, c, :, middle],
            fl_sem_s.at[cc], fl_sem_r.at[c], holder(2 * t + cc, sp),
        )

    def flow_from(cc):
        return remote(
            fl_v.at[pl.ds(0, 2)], field.at[0, cc, :, middle],
            fl_sem_s.at[cc], fl_sem_r.at[cc], at(cc, sp, tl),
        )

    @pl.when(flip == 0)
    def _():
        flow_copy(1 - c).start()

    @pl.when(flip == 1)
    def _():
        for cc in range(2):
            flow_copy(cc).start()

    def in_copy(k, side, e):
        cc, tt = peers[k]
        lanes = pl.ds(side * mid, mid)
        return remote(
            tr_v.at[:, 2 * pair_of(cc, tt) + e, :, lanes], stage.at[w, e, :, :, lanes],
            in_sem_s.at[k, side, e], in_sem_r.at[w, side, e], at(cc, sp, tt),
        )

    all_tr.wait()
    for k in (2, 0, 1):
        for side in range(2):
            for e in range(2):
                in_copy(k, side, e).start()

    def dep_copy(d):
        return remote(
            dep_v, depth_v.at[pl.ds(ROWS * (1 - d), ROWS)],
            dep_s.at[d + 1], dep_r.at[1 - d], holder(v, sp + d),
        )

    def relay_copy(d):
        return remote(
            field.at[0, :, :, middle], field.at[0, :, :, pl.ds(ROWS * (1 - d), ROWS)],
            rel_s.at[d + 1], rel_r.at[1 - d], holder(v, sp + d),
        )

    @pl.when(has_prev)
    def _():
        dep_copy(-1).start()

    @pl.when(has_next)
    def _():
        dep_copy(1).start()

    def halo_copy(wave, slot, d):
        low = d < 0
        step, lanes = (
            (0, pl.ds(0, mid)), (1, pl.ds(0, cut)), (1, pl.ds(cut, ny - cut)),
            (0, pl.ds(mid, ny - mid)),
        )[wave]
        return remote(
            grid.at[step, slot, pl.ds(GHOST if low else ROWS, GHOST), :, lanes],
            grid.at[step, slot, pl.ds(GHOST + ROWS if low else 0, GHOST), :, lanes],
            halo_s.at[wave, slot, 0 if low else 1], halo_r.at[wave, slot, 1 if low else 0],
            holder(v, sp + d),
        )

    def halo_start(wave, slot):
        @pl.when(has_prev)
        def _():
            halo_copy(wave, slot, -1).start()

        @pl.when(has_next)
        def _():
            halo_copy(wave, slot, 1).start()

    def halo_wait(wave, slot):
        @pl.when(has_prev)
        def _():
            halo_copy(wave, slot, 1).wait_recv()

        @pl.when(has_next)
        def _():
            halo_copy(wave, slot, -1).wait_recv()

    def halo_sent(wave, slot):
        @pl.when(has_prev)
        def _():
            halo_copy(wave, slot, -1).wait_send()

        @pl.when(has_next)
        def _():
            halo_copy(wave, slot, 1).wait_send()

    def regroup(slot, side):
        def tile(q, _):
            lanes = pl.ds(pl.multiple_of(q * 128, 128), 128)
            x = stage[slot, :, :, :, lanes].reshape(8, ROWS, 128)
            grid[0, slot, pl.ds(GHOST, ROWS), :, lanes] = jnp.swapaxes(x, 0, 1)
            return 0

        tiles = mid // 128
        lax.fori_loop(side * tiles, (side + 1) * tiles, tile, 0, unroll=2)

    def arrived(k):
        cc, tt = peers[k]
        slot = 2 * cc + tt
        for side in range(2):
            lanes = pl.ds(side * mid, mid)
            for e in range(2):
                remote(
                    stage.at[slot, e, :, :, lanes], stage.at[slot, e, :, :, lanes],
                    in_sem_s.at[k, side, e], in_sem_r.at[slot, side, e], at(cc, sp, tt),
                ).wait_recv()
            regroup(slot, side)
            halo_start(3 * side, slot)

    for copy in own_tr:
        copy.wait()
    for side in range(2):
        regroup(w, side)

    @pl.when(flip == 0)
    def _():
        my_flow.wait()
        flow_from(1 - c).wait_recv()

    @pl.when(flip == 1)
    def _():
        for cc in range(2):
            flow_from(cc).wait_recv()

    @pl.when(has_prev)
    def _():
        relay_copy(-1).start()

    @pl.when(has_next)
    def _():
        relay_copy(1).start()

    for side in range(2):
        halo_start(3 * side, w)
    arrived(2)

    @pl.when(has_prev)
    def _():
        dep_copy(1).wait_recv()
        relay_copy(1).wait_recv()

    @pl.when(has_next)
    def _():
        dep_copy(-1).wait_recv()
        relay_copy(-1).wait_recv()

    lane_deep = lax.broadcasted_iota(jnp.int32, (DEEP, ny), 1)
    top_half = lax.broadcasted_iota(jnp.int32, (8, ny), 0) < 4

    def wet_of(level, rows):
        return jnp.where(depth_v[rows] > level.astype(F32), 1.0, 0.0)

    def lap(a):
        left = jnp.where(lane_deep == 0, 0.0, roll_lanes(a, 1))
        right = jnp.where(lane_deep == ny - 1, 0.0, roll_lanes(a, -1))
        return pltpu.roll(a, 1, 0) + pltpu.roll(a, DEEP - 1, 0) + left + right - 4.0 * a

    def put_coefs(e, base, face):
        up = jnp.maximum(face, 0.0)
        down = jnp.minimum(face, 0.0)
        natural[e, base] = -COURANT * up
        natural[e, base + 1] = (-COURANT * 0.5) * up * (1.0 - COURANT * up)
        natural[e, base + 2] = -COURANT * down
        natural[e, base + 3] = (COURANT * 0.5) * down * (1.0 + COURANT * down)

    def spread_rows(ref, k, j):
        one = jnp.broadcast_to(ref[0, k, j : j + 1, :], (8, ny))
        two = jnp.broadcast_to(ref[1, k, j : j + 1, :], (8, ny))
        return jnp.where(top_half, one, two)

    def velocities(step, _):
        def level(e, _):
            wet = wet_of(2 * v + e, slice(None))
            u = field[step, 0, e]
            r = field[step, 1, e]
            u_new = wet * (u + CORIOLIS * r + VISCOSITY * lap(u) - FRICTION * u)
            r_new = wet * (r - CORIOLIS * u + VISCOSITY * lap(r) - FRICTION * r)
            field[step + 1, 0, e] = u_new
            field[step + 1, 1, e] = r_new
            face = 0.5 * (u_new + pltpu.roll(u_new, DEEP - 1, 0)) * wet * pltpu.roll(wet, DEEP - 1, 0)
            put_coefs(e, 0, face)
            wet_right = jnp.where(lane_deep == ny - 1, 0.0, roll_lanes(wet, -1))
            face = 0.5 * (r_new + roll_lanes(r_new, -1)) * wet * wet_right
            put_coefs(e, 4, face)
            return 0

        lax.fori_loop(0, 2, level, 0)
        shift = ROWS - GHOST
        for i in range(1, 14):
            for k in range(4):
                coef_x[step, i - 1, k] = spread_rows(natural, k, i + shift)
        for i in range(2, 14):
            for k in range(4):
                coef_y[step, i - 2, k] = spread_rows(natural, 4 + k, i + shift)
        return 0

    velocities(0, 0)

    def velocity_copy(comp):
        return remote(
            velocity_send.at[comp], flow_out.at[pl.ds(2 * c, 2)],
            fo_s.at[comp], fo_r.at[c], at(comp, sp, tl),
        )

    def velocity_from(cc):
        return remote(
            velocity_send.at[0], flow_out.at[pl.ds(2 * cc, 2)],
            fo_s.at[0], fo_r.at[cc], holder(2 * t + cc, sp),
        )

    velocity_own = pltpu.make_async_copy(
        velocity_send.at[c], flow_out.at[pl.ds(2 * c, 2)], fo_own.at[0]
    )

    def later_velocities():
        velocities(1, 0)
        own_rows = slice(ROWS, 2 * ROWS)
        above = jnp.where(v > 0, DIFFUSION, 0.0).astype(F32)
        wet_a = wet_of(2 * v, own_rows)
        wet_b = wet_of(2 * v + 1, own_rows)
        natural[0, 0, 0:ROWS] = DIFFUSION * wet_a * wet_b
        natural[1, 0, 0:ROWS] = DIFFUSION * wet_a * wet_b
        natural[0, 1, 0:ROWS] = above * wet_a * wet_of(2 * v - 1, own_rows)
        natural[1, 1, 0:ROWS] = DIFFUSION * wet_b * wet_of(2 * v + 2, own_rows)
        for row in range(ROWS):
            for k in range(2):
                mix_w[row, k] = spread_rows(natural, k, row)

        for comp in range(2):
            for e in range(2):
                velocity_send[comp, e] = field[STEPS, comp, e, own_rows]

        @pl.when(flip == 0)
        def _():
            velocity_own.start()
            velocity_copy(1 - c).start()

        @pl.when(flip == 1)
        def _():
            for comp in range(2):
                velocity_copy(comp).start()

    def along_x(step, load, first_face, last_face, start, size, put):
        def chunk(q, _):
            lanes = pl.ds(pl.multiple_of(start + q * PAIR, 128), PAIR)
            before = load(first_face - 1, lanes)
            here = load(first_face, lanes)
            ahead = load(first_face + 1, lanes)
            jump = ahead - here
            slope = limited(here - before, jump)
            last_flux = None
            for i in range(first_face, last_face + 1):
                far = load(i + 2, lanes)
                next_jump = far - ahead
                next_slope = limited(jump, next_jump)
                k = i - 1
                flux = (
                    coef_x[step, k, 0, :, lanes] * here
                    + coef_x[step, k, 1, :, lanes] * slope
                    + coef_x[step, k, 2, :, lanes] * ahead
                    + coef_x[step, k, 3, :, lanes] * next_slope
                )
                if last_flux is not None:
                    put(i, lanes, here, flux - last_flux)
                last_flux = flux
                here, ahead, jump, slope = ahead, far, next_jump, next_slope
            return 0

        lax.fori_loop(0, size // PAIR, chunk, 0, unroll=PAIRS)

    def along_y(step, i, a, lanes):
        columns = lax.broadcasted_iota(jnp.int32, a.shape, 1)
        right = jnp.where(columns == a.shape[1] - 1, 0.0, roll_lanes(a, -1))
        jump = right - a
        slope = limited(jnp.where(columns == 0, a, roll_lanes(jump, 1)), jump)
        flux = (
            coef_y[step, i - 2, 0, :, lanes] * a
            + coef_y[step, i - 2, 1, :, lanes] * slope
            + coef_y[step, i - 2, 2, :, lanes] * right
            + coef_y[step, i - 2, 3, :, lanes] * roll_lanes(slope, -1)
        )
        return flux - jnp.where(columns == 0, 0.0, roll_lanes(flux, 1))

    def advance(step, slot, start, size, keep_start, keep_size):
        lanes = pl.ds(start, size)
        kept = pl.ds(keep_start, keep_size)
        skip = keep_start - start

        def put_one(i, at_lanes, here, change):
            part[i, :, at_lanes] = here + change

        along_x(
            step, lambda i, at_lanes: grid[step, slot, i, :, at_lanes], 1, 13, start, size, put_one
        )

        def row_one(i, _):
            first[i, :, lanes] = part[i, :, lanes] + along_y(
                step, i, grid[step, slot, i, :, lanes], lanes
            )
            return 0

        lax.fori_loop(2, 14, row_one, 0, unroll=True)

        def put_two(i, at_lanes, here, change):
            part[i, :, at_lanes] = (grid[step, slot, i, :, at_lanes] + here) + change

        along_x(
            step, lambda i, at_lanes: first[i, :, at_lanes], 3, 11, keep_start, keep_size, put_two
        )

        def row_two(i, _):
            change = along_y(step, i, first[i, :, lanes], lanes)
            second[slot, i - GHOST, :, kept] = 0.5 * (
                part[i, :, kept] + change[:, skip : skip + keep_size]
            )
            return 0

        lax.fori_loop(GHOST, GHOST + ROWS, row_two, 0, unroll=True)

    def swap_halves(a):
        return pltpu.roll(a, 4, 0)

    kept_of = ((0, ny), (0, mid), (mid, ny - mid))

    def mix_copy(wave, slot, d):
        step, lanes = min(wave, 1), pl.ds(*kept_of[wave])
        return remote(
            packed.at[step, slot, 0 if d < 0 else 1, :, :, lanes],
            ext.at[step, 1 if d < 0 else 0, slot, :, :, lanes],
            mix_s.at[wave, slot, 0 if d < 0 else 1], mix_r.at[wave, slot, 1 if d < 0 else 0],
            holder(v + d, sp),
        )

    def mix_start(wave, slot):
        step, lanes = min(wave, 1), pl.ds(*kept_of[wave])
        in_top = lax.broadcasted_iota(jnp.int32, (8, kept_of[wave][1]), 0) < 4

        def row(i, _):
            a = second[slot, i, :, lanes]
            b = second[slot, i + HALF, :, lanes]
            packed[step, slot, 0, i, :, lanes] = jnp.where(in_top, a, swap_halves(b))
            packed[step, slot, 1, i, :, lanes] = jnp.where(in_top, swap_halves(a), b)
            return 0

        lax.fori_loop(0, HALF, row, 0, unroll=True)

        @pl.when(v > 0)
        def _():
            mix_copy(wave, slot, -1).start()

        @pl.when(v < 3)
        def _():
            mix_copy(wave, slot, 1).start()

    def mix_wait(wave, slot):
        @pl.when(v > 0)
        def _():
            mix_copy(wave, slot, 1).wait_recv()

        @pl.when(v < 3)
        def _():
            mix_copy(wave, slot, -1).wait_recv()

    def mix_sent(wave, slot):
        @pl.when(v > 0)
        def _():
            mix_copy(wave, slot, -1).wait_send()

        @pl.when(v < 3)
        def _():
            mix_copy(wave, slot, 1).wait_send()

    def settle(step, put, start, size):
        lanes = pl.ds(start, size)
        in_top = lax.broadcasted_iota(jnp.int32, (8, size), 0) < 4

        def reacted(i, beyond_of):
            inner = mix_w[i, 0, :, lanes]
            outer = mix_w[i, 1, :, lanes]
            mixed = []
            for slot in range(4):
                a = second[slot, i, :, lanes]
                beyond = beyond_of(slot)
                mixed.append(a + inner * (swap_halves(a) - a) + outer * (beyond - a))
            whole = jnp.concatenate(mixed, axis=0)
            soft = whole / (1.0 + jnp.abs(whole))
            done = whole + jnp.dot(
                matrix[...], soft, precision=lax.Precision.HIGHEST, preferred_element_type=F32
            )
            for slot in range(4):
                put(slot, i, lanes, done[8 * slot : 8 * slot + 8])

        def rows(j, _):
            reacted(
                j,
                lambda slot: jnp.where(
                    in_top,
                    ext[step, 0, slot, j, :, lanes],
                    swap_halves(ext[step, 1, slot, j, :, lanes]),
                ),
            )
            reacted(
                j + HALF,
                lambda slot: jnp.where(
                    in_top,
                    swap_halves(ext[step, 0, slot, j, :, lanes]),
                    ext[step, 1, slot, j, :, lanes],
                ),
            )
            return 0

        lax.fori_loop(0, HALF, rows, 0)

    between = jnp.logical_or(
        jnp.logical_and(has_prev, odd(sp - 1) != flip),
        jnp.logical_and(has_next, odd(sp + 1) != flip),
    )
    near, far, last = 2 * (1 - c) + t, 2 * c + 1 - t, 2 * (1 - c) + 1 - t
    order = [
        jnp.where(between, far, w), jnp.where(between, last, near), jnp.where(between, w, far),
        jnp.where(between, near, last),
    ]

    arrived(0)

    @pl.when(between)
    def _():
        arrived(1)

    for number, slot in enumerate(order):
        if number == 2:

            @pl.when(jnp.logical_not(between))
            def _():
                arrived(1)

        if number == 3:
            later_velocities()
        halo_wait(0, slot)
        halo_wait(3, slot)
        advance(0, slot, 0, ny, 0, ny)
        mix_start(0, slot)
    for slot in range(4):
        mix_wait(0, slot)

    def put_next(slot, i, lanes, a):
        grid[1, slot, GHOST + i, :, lanes] = a

    for wave, (start, size) in ((1, (0, cut)), (2, (cut, ny - cut))):
        settle(0, put_next, start, size)
        for slot in range(4):
            halo_start(wave, slot)

    def put_final(slot, i, lanes, a):
        final[slot, i, :, lanes] = a

    def out_copy(k, wave):
        cc, tt = peers[k]
        lanes = pl.ds(*kept_of[wave])
        return remote(
            final.at[2 * cc + tt, :, :, lanes], out.at[v, :, :, lanes],
            out_s.at[k, wave], out_r.at[v, wave], at(cc, sp, tt),
        )

    def out_from(k, wave):
        cc, tt = peers[k]
        lanes = pl.ds(*kept_of[wave])
        source = pair_of(cc, tt)
        return remote(
            final.at[w, :, :, lanes], out.at[source, :, :, lanes],
            out_s.at[k, wave], out_r.at[source, wave], at(cc, sp, tt),
        )

    def own_copy(wave):
        lanes = pl.ds(*kept_of[wave])
        return pltpu.make_async_copy(
            final.at[w, :, :, lanes], out.at[v, :, :, lanes], own_out.at[wave]
        )

    def window(wave, slots):
        def one(slot, _):
            halo_wait(wave, slot)
            start = (0, ny - width)[wave - 1]
            advance(1, slot, start, width, *kept_of[wave])
            mix_start(wave, slot)
            return 0

        lax.fori_loop(*slots, one, 0)

    def finish(wave):
        for slot in range(4):
            mix_wait(wave, slot)
        settle(1, put_final, *kept_of[wave])
        for k in range(3):
            out_copy(k, wave).start()
        own_copy(wave).start()

    window(1, (0, 4))
    window(2, (0, 2))
    finish(1)
    window(2, (2, 4))
    finish(2)

    for wave in (1, 2):
        own_copy(wave).wait()

    @pl.when(flip == 0)
    def _():
        velocity_own.wait()
        velocity_copy(1 - c).wait_send()
        velocity_from(1 - c).wait_recv()
        flow_copy(1 - c).wait_send()

    @pl.when(flip == 1)
    def _():
        for cc in range(2):
            velocity_copy(cc).wait_send()
            velocity_from(cc).wait_recv()
            flow_copy(cc).wait_send()

    for k in range(3):
        for side in range(2):
            for e in range(2):
                in_copy(k, side, e).wait_send()

    @pl.when(has_prev)
    def _():
        dep_copy(-1).wait_send()
        relay_copy(-1).wait_send()

    @pl.when(has_next)
    def _():
        dep_copy(1).wait_send()
        relay_copy(1).wait_send()

    for slot in range(4):
        for wave in range(4):
            halo_sent(wave, slot)
        for wave in range(3):
            mix_sent(wave, slot)
    for wave in (1, 2):
        for k in range(3):
            out_copy(k, wave).wait_send()
            out_from(k, wave).wait_recv()


def place(blocks, flow, out, flow_out, held, held_flow, ready, sems):
    ny = blocks.shape[-1]
    loads = [pltpu.make_async_copy(blocks.at[g], held.at[g], sems.at[5 + g]) for g in range(4)]
    for load in loads:
        load.start()
    flow_in = pltpu.make_async_copy(flow, held_flow, sems.at[9])
    flow_in.start()
    copies = []
    for pair in range(4):
        loads[pair].wait()

        def tile(q, _):
            lanes = pl.ds(pl.multiple_of(q * 128, 128), 128)
            x = jnp.swapaxes(held[pair, :, :, lanes], 0, 1)
            for e in range(2):
                for s in range(4):
                    ready[pair, s, e, :, lanes] = x[4 * e + s]
            return 0

        lax.fori_loop(0, ny // 128, tile, 0, unroll=4)
        copy = pltpu.make_async_copy(ready.at[pair], out.at[:, pl.ds(2 * pair, 2)], sems.at[pair])
        copy.start()
        copies.append(copy)
    flow_in.wait()
    flow_copy = pltpu.make_async_copy(held_flow, flow_out, sems.at[4])
    flow_copy.start()
    for copy in copies:
        copy.wait()
    flow_copy.wait()


def body(tracers, flow, reaction_rates, land_mask, layers):
    ny = tracers.shape[-1]
    vmem = pl.BlockSpec(memory_space=pltpu.VMEM)
    anywhere = pl.BlockSpec(memory_space=pl.ANY)
    dma = pltpu.SemaphoreType.DMA
    blocks, flow_done = pl.pallas_call(
        kernel,
        out_shape=(
            jax.ShapeDtypeStruct((4, ROWS, 8, ny), F32),
            jax.ShapeDtypeStruct((4, ROWS, ny), F32),
        ),
        in_specs=[pl.BlockSpec(memory_space=pltpu.HBM)] * 2 + [vmem] * 3,
        out_specs=(anywhere, anywhere),
        scratch_shapes=[
            pltpu.VMEM((4, 8, ROWS, ny), F32),
            pltpu.VMEM((4, ROWS, ny), F32),
            pltpu.VMEM((ROWS, ny), F32),
            pltpu.VMEM((32, 32), F32),
            pltpu.VMEM((4, 2, 4, ROWS, ny), F32),
            pltpu.VMEM((STEPS, 4, SPAN, 8, ny), F32),
            pltpu.VMEM((SPAN, 8, ny), F32),
            pltpu.VMEM((SPAN, 8, ny), F32),
            pltpu.VMEM((4, ROWS, 8, ny), F32),
            pltpu.VMEM((STEPS, 13, 4, 8, ny), F32),
            pltpu.VMEM((STEPS, 12, 4, 8, ny), F32),
            pltpu.VMEM((ROWS, 2, 8, ny), F32),
            pltpu.VMEM((2, 8, DEEP, ny), F32),
            pltpu.VMEM((STEPS + 1, 2, 2, DEEP, ny), F32),
            pltpu.VMEM((DEEP, ny), F32),
            pltpu.VMEM((STEPS, 4, 2, HALF, 8, ny), F32),
            pltpu.VMEM((STEPS, 2, 4, HALF, 8, ny), F32),
            pltpu.VMEM((4, ROWS, 8, ny), F32),
            pltpu.VMEM((2, 2, ROWS, ny), F32),
            dma((3,)), dma((3, 2, 2)), dma((4, 2, 2)),
            dma((2,)), dma((2,)), dma((2,)), dma((3,)), dma((3,)), dma((3,)), dma((3,)),
            dma((4, 4, 2)), dma((4, 4, 2)),
            dma((3, 4, 2)), dma((3, 4, 2)),
            dma((3, 3)), dma((4, 3)), dma((3,)),
            dma((2,)), dma((2,)), dma((1,)),
        ],
        compiler_params=pltpu.CompilerParams(
            collective_id=0, has_side_effects=True, vmem_limit_bytes=ALL_VMEM
        ),
        name="ocean",
    )(tracers, flow, reaction_rates, land_mask, layers)
    return pl.pallas_call(
        place,
        out_shape=(
            jax.ShapeDtypeStruct(tracers.shape, F32),
            jax.ShapeDtypeStruct(flow.shape, F32),
        ),
        in_specs=[pl.BlockSpec(memory_space=pltpu.HBM)] * 2,
        out_specs=(pl.BlockSpec(memory_space=pltpu.HBM),) * 2,
        scratch_shapes=[
            pltpu.VMEM((4, ROWS, 8, ny), F32),
            pltpu.VMEM((4, ROWS, ny), F32),
            pltpu.VMEM((4, 4, 2, ROWS, ny), F32),
            dma((10,)),
        ],
        compiler_params=pltpu.CompilerParams(vmem_limit_bytes=ALL_VMEM),
        name="place",
    )(blocks, flow_done)


def solution(mesh):
    placed = (
        P(("comp", "trc"), None, "space", None),
        P(("comp", "trc"), "space", None),
        P(),
        P("space", None),
        P("space", None),
    )
    return jax.shard_map(
        body,
        mesh=mesh,
        in_specs=placed,
        out_specs=(P(("comp", "trc"), None, "space", None), P(("comp", "trc"), "space", None)),
        check_vma=False,
    )
```

```python
import functools

import jax
import jax.numpy as jnp
from jax import lax
from jax.experimental import pallas as pl
from jax.experimental.pallas import tpu as pltpu
from jax.sharding import PartitionSpec as P

STEPS = 2
COURANT = 0.25
VISCOSITY = 0.2
CORIOLIS = 0.3
FRICTION = 0.1
DIFFUSION = 0.3
REACT_STEP = 0.5

MESH = pl.DeviceIdType.MESH
F32 = jnp.float32
ROWS = 8
DEEP = 24
GHOST = 4
SPAN = ROWS + 2 * GHOST
EDGE = 128
HALF = ROWS // 2
ALL_VMEM = 67_043_328
LINE = 8
PAIR = 128
PAIRS = 2


def limited(before, after):
    return jnp.maximum(jnp.minimum(after, 0.0), jnp.minimum(before, jnp.maximum(after, 0.0)))


def roll_lanes(a, by):
    return pltpu.roll(a, by % a.shape[-1], a.ndim - 1)


def kernel(
    tracers, flow, rates, land, layers, out, flow_out,
    tr_v, fl_v, dep_v, matrix, stage, grid, first, part, second, coef_x, coef_y, mix_w, natural,
    field, depth_v, packed, ext, final, velocity_send,
    in_local, in_sem_s, in_sem_r, fl_local, fl_sem_s, fl_sem_r, rel_s, rel_r, dep_s, dep_r,
    halo_s, halo_r, mix_s, mix_r, out_s, out_r, own_out, fo_s, fo_r, fo_own,
):
    ny = tracers.shape[-1]
    c = lax.axis_index("comp")
    sp = lax.axis_index("space")
    t = lax.axis_index("trc")
    n = lax.axis_size("space")
    w = 2 * c + t
    has_prev = sp > 0
    has_next = sp < n - 1

    def odd(strip):
        return lax.rem(strip // LINE, 2)

    def flipped(bit, strip):
        return lax.rem(bit + odd(strip), 2)

    flip = odd(sp)
    tl = flipped(t, sp)
    v = 2 * tl + c

    def at(cc, ss, tt):
        return {"comp": cc, "space": ss, "trc": tt}

    def holder(pair, strip):
        return at(lax.rem(pair, 2), strip, flipped(pair // 2, strip))

    def remote(src, dst, s, r, dev):
        return pltpu.make_async_remote_copy(
            src_ref=src, dst_ref=dst, send_sem=s, recv_sem=r, device_id=dev, device_id_type=MESH
        )

    middle = pl.ds(ROWS, ROWS)
    mid = ny // 2
    cut = mid + EDGE
    width = mid + EDGE

    all_flow = pltpu.make_async_copy(flow, fl_v, fl_local.at[1])
    all_tr = pltpu.make_async_copy(tracers, tr_v, in_local.at[0])
    own_tr = [
        pltpu.make_async_copy(tracers.at[:, 2 * v + e], stage.at[w, e], in_local.at[1 + e])
        for e in range(2)
    ]
    my_flow = pltpu.make_async_copy(
        flow.at[pl.ds(2 * c, 2)], field.at[0, c, :, middle], fl_local.at[0]
    )
    all_flow.start()
    all_tr.start()
    for copy in own_tr:
        copy.start()

    @pl.when(flip == 0)
    def _():
        my_flow.start()

    barrier = pltpu.get_barrier_semaphore()
    peers = [(c, 1 - t), (1 - c, 1 - t), (1 - c, t)]

    def pair_of(cc, tt):
        return 2 * flipped(tt, sp) + cc

    for cc, tt in peers:
        pl.semaphore_signal(barrier, inc=1, device_id=at(cc, sp, tt), device_id_type=MESH)

    @pl.when(has_prev)
    def _():
        pl.semaphore_signal(barrier, inc=1, device_id=holder(v, sp - 1), device_id_type=MESH)

    @pl.when(has_next)
    def _():
        pl.semaphore_signal(barrier, inc=1, device_id=holder(v, sp + 1), device_id_type=MESH)

    dep_v[...] = jnp.where(land[...] > 0, layers[...], 0).astype(F32)
    depth_v[middle] = dep_v[...]

    @pl.when(jnp.logical_not(has_prev))
    def _():
        depth_v[0:ROWS] = jnp.zeros((ROWS, ny), F32)
        for comp in range(2):
            for e in range(2):
                field[0, comp, e, 0:ROWS] = jnp.zeros((ROWS, ny), F32)
        for step in range(2):
            for slot in range(4):
                for row in range(GHOST):
                    grid[step, slot, row] = jnp.zeros((8, ny), F32)

    @pl.when(jnp.logical_not(has_next))
    def _():
        depth_v[2 * ROWS :] = jnp.zeros((ROWS, ny), F32)
        for comp in range(2):
            for e in range(2):
                field[0, comp, e, 2 * ROWS :] = jnp.zeros((ROWS, ny), F32)
        for step in range(2):
            for slot in range(4):
                for row in range(GHOST):
                    grid[step, slot, GHOST + ROWS + row] = jnp.zeros((8, ny), F32)

    @pl.when(v == 0)
    def _():
        for step in range(2):
            for slot in range(4):
                ext[step, 0, slot] = jnp.zeros((HALF, 8, ny), F32)

    @pl.when(v == 3)
    def _():
        for step in range(2):
            for slot in range(4):
                ext[step, 1, slot] = jnp.zeros((HALF, 8, ny), F32)

    lines = lax.broadcasted_iota(jnp.int32, (32, 16), 0)
    names = lax.broadcasted_iota(jnp.int32, (32, 16), 1)
    pick = jnp.where(4 * (lines // 8) + lax.rem(lines, 4) == names, 1.0, 0.0)
    wide = jnp.dot(pick, rates[...], precision=lax.Precision.HIGHEST, preferred_element_type=F32)
    wide = lax.dot_general(
        wide, pick, (((1,), (1,)), ((), ())),
        precision=lax.Precision.HIGHEST, preferred_element_type=F32,
    )
    line = lax.broadcasted_iota(jnp.int32, (32, 32), 0)
    other = lax.broadcasted_iota(jnp.int32, (32, 32), 1)
    same_level = lax.rem(line // 4, 2) == lax.rem(other // 4, 2)
    matrix[...] = jnp.where(same_level, REACT_STEP * wide, 0.0)

    all_flow.wait()
    pl.semaphore_wait(barrier, 3 + jnp.where(has_prev, 1, 0) + jnp.where(has_next, 1, 0))

    def flow_copy(cc):
        return remote(
            fl_v.at[pl.ds(2 * cc, 2)], field.at[0, c, :, middle],
            fl_sem_s.at[cc], fl_sem_r.at[c], holder(2 * t + cc, sp),
        )

    def flow_from(cc):
        return remote(
            fl_v.at[pl.ds(0, 2)], field.at[0, cc, :, middle],
            fl_sem_s.at[cc], fl_sem_r.at[cc], at(cc, sp, tl),
        )

    @pl.when(flip == 0)
    def _():
        flow_copy(1 - c).start()

    @pl.when(flip == 1)
    def _():
        for cc in range(2):
            flow_copy(cc).start()

    def in_copy(k, side, e):
        cc, tt = peers[k]
        lanes = pl.ds(side * mid, mid)
        return remote(
            tr_v.at[:, 2 * pair_of(cc, tt) + e, :, lanes], stage.at[w, e, :, :, lanes],
            in_sem_s.at[k, side, e], in_sem_r.at[w, side, e], at(cc, sp, tt),
        )

    all_tr.wait()
    for k in (2, 0, 1):
        for side in range(2):
            for e in range(2):
                in_copy(k, side, e).start()

    def dep_copy(d):
        return remote(
            dep_v, depth_v.at[pl.ds(ROWS * (1 - d), ROWS)],
            dep_s.at[d + 1], dep_r.at[1 - d], holder(v, sp + d),
        )

    def relay_copy(d):
        return remote(
            field.at[0, :, :, middle], field.at[0, :, :, pl.ds(ROWS * (1 - d), ROWS)],
            rel_s.at[d + 1], rel_r.at[1 - d], holder(v, sp + d),
        )

    @pl.when(has_prev)
    def _():
        dep_copy(-1).start()

    @pl.when(has_next)
    def _():
        dep_copy(1).start()

    def halo_copy(wave, slot, d):
        low = d < 0
        step, lanes = (
            (0, pl.ds(0, mid)), (1, pl.ds(0, cut)), (1, pl.ds(cut, ny - cut)),
            (0, pl.ds(mid, ny - mid)),
        )[wave]
        return remote(
            grid.at[step, slot, pl.ds(GHOST if low else ROWS, GHOST), :, lanes],
            grid.at[step, slot, pl.ds(GHOST + ROWS if low else 0, GHOST), :, lanes],
            halo_s.at[wave, slot, 0 if low else 1], halo_r.at[wave, slot, 1 if low else 0],
            holder(v, sp + d),
        )

    def halo_start(wave, slot):
        @pl.when(has_prev)
        def _():
            halo_copy(wave, slot, -1).start()

        @pl.when(has_next)
        def _():
            halo_copy(wave, slot, 1).start()

    def halo_wait(wave, slot):
        @pl.when(has_prev)
        def _():
            halo_copy(wave, slot, 1).wait_recv()

        @pl.when(has_next)
        def _():
            halo_copy(wave, slot, -1).wait_recv()

    def halo_sent(wave, slot):
        @pl.when(has_prev)
        def _():
            halo_copy(wave, slot, -1).wait_send()

        @pl.when(has_next)
        def _():
            halo_copy(wave, slot, 1).wait_send()

    def regroup(slot, side):
        def tile(q, _):
            lanes = pl.ds(pl.multiple_of(q * 128, 128), 128)
            x = stage[slot, :, :, :, lanes].reshape(8, ROWS, 128)
            grid[0, slot, pl.ds(GHOST, ROWS), :, lanes] = jnp.swapaxes(x, 0, 1)
            return 0

        tiles = mid // 128
        lax.fori_loop(side * tiles, (side + 1) * tiles, tile, 0, unroll=2)

    def arrived(k):
        cc, tt = peers[k]
        slot = 2 * cc + tt
        for side in range(2):
            lanes = pl.ds(side * mid, mid)
            for e in range(2):
                remote(
                    stage.at[slot, e, :, :, lanes], stage.at[slot, e, :, :, lanes],
                    in_sem_s.at[k, side, e], in_sem_r.at[slot, side, e], at(cc, sp, tt),
                ).wait_recv()
            regroup(slot, side)
            halo_start(3 * side, slot)

    for copy in own_tr:
        copy.wait()
    for side in range(2):
        regroup(w, side)

    @pl.when(flip == 0)
    def _():
        my_flow.wait()
        flow_from(1 - c).wait_recv()

    @pl.when(flip == 1)
    def _():
        for cc in range(2):
            flow_from(cc).wait_recv()

    @pl.when(has_prev)
    def _():
        relay_copy(-1).start()

    @pl.when(has_next)
    def _():
        relay_copy(1).start()

    for side in range(2):
        halo_start(3 * side, w)
    arrived(2)

    @pl.when(has_prev)
    def _():
        dep_copy(1).wait_recv()
        relay_copy(1).wait_recv()

    @pl.when(has_next)
    def _():
        dep_copy(-1).wait_recv()
        relay_copy(-1).wait_recv()

    lane_deep = lax.broadcasted_iota(jnp.int32, (DEEP, ny), 1)
    top_half = lax.broadcasted_iota(jnp.int32, (8, ny), 0) < 4

    def wet_of(level, rows):
        return jnp.where(depth_v[rows] > level.astype(F32), 1.0, 0.0)

    def lap(a):
        left = jnp.where(lane_deep == 0, 0.0, roll_lanes(a, 1))
        right = jnp.where(lane_deep == ny - 1, 0.0, roll_lanes(a, -1))
        return pltpu.roll(a, 1, 0) + pltpu.roll(a, DEEP - 1, 0) + left + right - 4.0 * a

    def put_coefs(e, base, face):
        up = jnp.maximum(face, 0.0)
        down = jnp.minimum(face, 0.0)
        natural[e, base] = -COURANT * up
        natural[e, base + 1] = (-COURANT * 0.5) * up * (1.0 - COURANT * up)
        natural[e, base + 2] = -COURANT * down
        natural[e, base + 3] = (COURANT * 0.5) * down * (1.0 + COURANT * down)

    def spread_rows(ref, k, j):
        one = jnp.broadcast_to(ref[0, k, j : j + 1, :], (8, ny))
        two = jnp.broadcast_to(ref[1, k, j : j + 1, :], (8, ny))
        return jnp.where(top_half, one, two)

    def velocities(step, _):
        def level(e, _):
            wet = wet_of(2 * v + e, slice(None))
            u = field[step, 0, e]
            r = field[step, 1, e]
            u_new = wet * (u + CORIOLIS * r + VISCOSITY * lap(u) - FRICTION * u)
            r_new = wet * (r - CORIOLIS * u + VISCOSITY * lap(r) - FRICTION * r)
            field[step + 1, 0, e] = u_new
            field[step + 1, 1, e] = r_new
            face = 0.5 * (u_new + pltpu.roll(u_new, DEEP - 1, 0)) * wet * pltpu.roll(wet, DEEP - 1, 0)
            put_coefs(e, 0, face)
            wet_right = jnp.where(lane_deep == ny - 1, 0.0, roll_lanes(wet, -1))
            face = 0.5 * (r_new + roll_lanes(r_new, -1)) * wet * wet_right
            put_coefs(e, 4, face)
            return 0

        lax.fori_loop(0, 2, level, 0)
        shift = ROWS - GHOST
        for i in range(1, 14):
            for k in range(4):
                coef_x[step, i - 1, k] = spread_rows(natural, k, i + shift)
        for i in range(2, 14):
            for k in range(4):
                coef_y[step, i - 2, k] = spread_rows(natural, 4 + k, i + shift)
        return 0

    velocities(0, 0)

    def velocity_copy(comp):
        return remote(
            velocity_send.at[comp], flow_out.at[pl.ds(2 * c, 2)],
            fo_s.at[comp], fo_r.at[c], at(comp, sp, tl),
        )

    def velocity_from(cc):
        return remote(
            velocity_send.at[0], flow_out.at[pl.ds(2 * cc, 2)],
            fo_s.at[0], fo_r.at[cc], holder(2 * t + cc, sp),
        )

    velocity_own = pltpu.make_async_copy(
        velocity_send.at[c], flow_out.at[pl.ds(2 * c, 2)], fo_own.at[0]
    )

    own_rows = slice(ROWS, 2 * ROWS)

    def mixing_weights():
        above = jnp.where(v > 0, DIFFUSION, 0.0).astype(F32)
        wet_a = wet_of(2 * v, own_rows)
        wet_b = wet_of(2 * v + 1, own_rows)
        natural[0, 0, 0:ROWS] = DIFFUSION * wet_a * wet_b
        natural[1, 0, 0:ROWS] = DIFFUSION * wet_a * wet_b
        natural[0, 1, 0:ROWS] = above * wet_a * wet_of(2 * v - 1, own_rows)
        natural[1, 1, 0:ROWS] = DIFFUSION * wet_b * wet_of(2 * v + 2, own_rows)
        for row in range(ROWS):
            for k in range(2):
                mix_w[row, k] = spread_rows(natural, k, row)


    def send_velocities():
        for comp in range(2):
            for e in range(2):
                velocity_send[comp, e] = field[STEPS, comp, e, own_rows]

        @pl.when(flip == 0)
        def _():
            velocity_own.start()
            velocity_copy(1 - c).start()

        @pl.when(flip == 1)
        def _():
            for comp in range(2):
                velocity_copy(comp).start()

    def along_x(step, load, first_face, last_face, start, size, put):
        def chunk(q, _):
            lanes = pl.ds(pl.multiple_of(start + q * PAIR, 128), PAIR)
            before = load(first_face - 1, lanes)
            here = load(first_face, lanes)
            ahead = load(first_face + 1, lanes)
            jump = ahead - here
            slope = limited(here - before, jump)
            last_flux = None
            for i in range(first_face, last_face + 1):
                far = load(i + 2, lanes)
                next_jump = far - ahead
                next_slope = limited(jump, next_jump)
                k = i - 1
                flux = (
                    coef_x[step, k, 0, :, lanes] * here
                    + coef_x[step, k, 1, :, lanes] * slope
                    + coef_x[step, k, 2, :, lanes] * ahead
                    + coef_x[step, k, 3, :, lanes] * next_slope
                )
                if last_flux is not None:
                    put(i, lanes, here, flux - last_flux)
                last_flux = flux
                here, ahead, jump, slope = ahead, far, next_jump, next_slope
            return 0

        lax.fori_loop(0, size // PAIR, chunk, 0, unroll=PAIRS)

    def along_y(step, i, a, lanes):
        columns = lax.broadcasted_iota(jnp.int32, a.shape, 1)
        right = jnp.where(columns == a.shape[1] - 1, 0.0, roll_lanes(a, -1))
        jump = right - a
        slope = limited(jnp.where(columns == 0, a, roll_lanes(jump, 1)), jump)
        flux = (
            coef_y[step, i - 2, 0, :, lanes] * a
            + coef_y[step, i - 2, 1, :, lanes] * slope
            + coef_y[step, i - 2, 2, :, lanes] * right
            + coef_y[step, i - 2, 3, :, lanes] * roll_lanes(slope, -1)
        )
        return flux - jnp.where(columns == 0, 0.0, roll_lanes(flux, 1))

    def advance(step, slot, start, size, keep_start, keep_size):
        lanes = pl.ds(start, size)
        kept = pl.ds(keep_start, keep_size)
        skip = keep_start - start

        def put_one(i, at_lanes, here, change):
            part[i, :, at_lanes] = here + change

        along_x(
            step, lambda i, at_lanes: grid[step, slot, i, :, at_lanes], 1, 13, start, size, put_one
        )

        def row_one(i, _):
            first[i, :, lanes] = part[i, :, lanes] + along_y(
                step, i, grid[step, slot, i, :, lanes], lanes
            )
            return 0

        lax.fori_loop(2, 14, row_one, 0, unroll=True)

        def put_two(i, at_lanes, here, change):
            part[i, :, at_lanes] = (grid[step, slot, i, :, at_lanes] + here) + change

        along_x(
            step, lambda i, at_lanes: first[i, :, at_lanes], 3, 11, keep_start, keep_size, put_two
        )

        def row_two(i, _):
            change = along_y(step, i, first[i, :, lanes], lanes)
            second[slot, i - GHOST, :, kept] = 0.5 * (
                part[i, :, kept] + change[:, skip : skip + keep_size]
            )
            return 0

        lax.fori_loop(GHOST, GHOST + ROWS, row_two, 0, unroll=True)

    def swap_halves(a):
        return pltpu.roll(a, 4, 0)

    kept_of = ((0, ny), (0, mid), (mid, ny - mid))

    def mix_copy(wave, slot, d):
        step, lanes = min(wave, 1), pl.ds(*kept_of[wave])
        return remote(
            packed.at[step, slot, 0 if d < 0 else 1, :, :, lanes],
            ext.at[step, 1 if d < 0 else 0, slot, :, :, lanes],
            mix_s.at[wave, slot, 0 if d < 0 else 1], mix_r.at[wave, slot, 1 if d < 0 else 0],
            holder(v + d, sp),
        )

    def mix_start(wave, slot):
        step, lanes = min(wave, 1), pl.ds(*kept_of[wave])
        in_top = lax.broadcasted_iota(jnp.int32, (8, kept_of[wave][1]), 0) < 4

        def row(i, _):
            a = second[slot, i, :, lanes]
            b = second[slot, i + HALF, :, lanes]
            packed[step, slot, 0, i, :, lanes] = jnp.where(in_top, a, swap_halves(b))
            packed[step, slot, 1, i, :, lanes] = jnp.where(in_top, swap_halves(a), b)
            return 0

        lax.fori_loop(0, HALF, row, 0, unroll=True)

        @pl.when(v > 0)
        def _():
            mix_copy(wave, slot, -1).start()

        @pl.when(v < 3)
        def _():
            mix_copy(wave, slot, 1).start()

    def mix_wait(wave, slot):
        @pl.when(v > 0)
        def _():
            mix_copy(wave, slot, 1).wait_recv()

        @pl.when(v < 3)
        def _():
            mix_copy(wave, slot, -1).wait_recv()

    def mix_sent(wave, slot):
        @pl.when(v > 0)
        def _():
            mix_copy(wave, slot, -1).wait_send()

        @pl.when(v < 3)
        def _():
            mix_copy(wave, slot, 1).wait_send()

    def settle(step, put, start, size):
        lanes = pl.ds(start, size)
        in_top = lax.broadcasted_iota(jnp.int32, (8, size), 0) < 4

        def reacted(i, beyond_of):
            inner = mix_w[i, 0, :, lanes]
            outer = mix_w[i, 1, :, lanes]
            mixed = []
            for slot in range(4):
                a = second[slot, i, :, lanes]
                beyond = beyond_of(slot)
                mixed.append(a + inner * (swap_halves(a) - a) + outer * (beyond - a))
            whole = jnp.concatenate(mixed, axis=0)
            soft = whole / (1.0 + jnp.abs(whole))
            done = whole + jnp.dot(
                matrix[...], soft, precision=lax.Precision.HIGHEST, preferred_element_type=F32
            )
            for slot in range(4):
                put(slot, i, lanes, done[8 * slot : 8 * slot + 8])

        def rows(j, _):
            reacted(
                j,
                lambda slot: jnp.where(
                    in_top,
                    ext[step, 0, slot, j, :, lanes],
                    swap_halves(ext[step, 1, slot, j, :, lanes]),
                ),
            )
            reacted(
                j + HALF,
                lambda slot: jnp.where(
                    in_top,
                    swap_halves(ext[step, 0, slot, j, :, lanes]),
                    ext[step, 1, slot, j, :, lanes],
                ),
            )
            return 0

        lax.fori_loop(0, HALF, rows, 0, unroll=2)

    between = jnp.logical_or(
        jnp.logical_and(has_prev, odd(sp - 1) != flip),
        jnp.logical_and(has_next, odd(sp + 1) != flip),
    )
    near, far, last = 2 * (1 - c) + t, 2 * c + 1 - t, 2 * (1 - c) + 1 - t
    order = [
        jnp.where(between, far, w), jnp.where(between, last, near), jnp.where(between, w, far),
        jnp.where(between, near, last),
    ]

    arrived(0)

    @pl.when(between)
    def _():
        arrived(1)

    for number, slot in enumerate(order):
        if number == 2:

            @pl.when(jnp.logical_not(between))
            def _():
                arrived(1)

        if number == 3:
            velocities(1, 0)
        halo_wait(0, slot)
        halo_wait(3, slot)
        advance(0, slot, 0, ny, 0, ny)
        mix_start(0, slot)
    mixing_weights()
    for slot in range(4):
        mix_wait(0, slot)

    def put_next(slot, i, lanes, a):
        grid[1, slot, GHOST + i, :, lanes] = a

    for wave, (start, size) in ((1, (0, cut)), (2, (cut, ny - cut))):
        settle(0, put_next, start, size)
        for slot in range(4):
            halo_start(wave, slot)

    send_velocities()

    def put_final(slot, i, lanes, a):
        final[slot, i, :, lanes] = a

    def out_copy(k, wave):
        cc, tt = peers[k]
        lanes = pl.ds(*kept_of[wave])
        return remote(
            final.at[2 * cc + tt, :, :, lanes], out.at[v, :, :, lanes],
            out_s.at[k, wave], out_r.at[v, wave], at(cc, sp, tt),
        )

    def out_from(k, wave):
        cc, tt = peers[k]
        lanes = pl.ds(*kept_of[wave])
        source = pair_of(cc, tt)
        return remote(
            final.at[w, :, :, lanes], out.at[source, :, :, lanes],
            out_s.at[k, wave], out_r.at[source, wave], at(cc, sp, tt),
        )

    def own_copy(wave):
        lanes = pl.ds(*kept_of[wave])
        return pltpu.make_async_copy(
            final.at[w, :, :, lanes], out.at[v, :, :, lanes], own_out.at[wave]
        )

    def window(wave, slots):
        def one(slot, _):
            halo_wait(wave, slot)
            start = (0, ny - width)[wave - 1]
            advance(1, slot, start, width, *kept_of[wave])
            mix_start(wave, slot)
            return 0

        lax.fori_loop(*slots, one, 0)

    def finish(wave):
        for slot in range(4):
            mix_wait(wave, slot)
        settle(1, put_final, *kept_of[wave])
        for k in range(3):
            out_copy(k, wave).start()
        own_copy(wave).start()

    window(1, (0, 4))
    window(2, (0, 4))
    finish(1)
    finish(2)

    for wave in (1, 2):
        own_copy(wave).wait()

    @pl.when(flip == 0)
    def _():
        velocity_own.wait()
        velocity_copy(1 - c).wait_send()
        velocity_from(1 - c).wait_recv()
        flow_copy(1 - c).wait_send()

    @pl.when(flip == 1)
    def _():
        for cc in range(2):
            velocity_copy(cc).wait_send()
            velocity_from(cc).wait_recv()
            flow_copy(cc).wait_send()

    for k in range(3):
        for side in range(2):
            for e in range(2):
                in_copy(k, side, e).wait_send()

    @pl.when(has_prev)
    def _():
        dep_copy(-1).wait_send()
        relay_copy(-1).wait_send()

    @pl.when(has_next)
    def _():
        dep_copy(1).wait_send()
        relay_copy(1).wait_send()

    for slot in range(4):
        for wave in range(4):
            halo_sent(wave, slot)
        for wave in range(3):
            mix_sent(wave, slot)
    for wave in (1, 2):
        for k in range(3):
            out_copy(k, wave).wait_send()
            out_from(k, wave).wait_recv()


def place(blocks, flow, out, flow_out, held, held_flow, ready, sems):
    ny = blocks.shape[-1]
    loads = [pltpu.make_async_copy(blocks.at[g], held.at[g], sems.at[5 + g]) for g in range(4)]
    for load in loads:
        load.start()
    flow_in = pltpu.make_async_copy(flow, held_flow, sems.at[9])
    flow_in.start()
    copies = []
    for pair in range(4):
        loads[pair].wait()

        def tile(q, _):
            lanes = pl.ds(pl.multiple_of(q * 128, 128), 128)
            x = jnp.swapaxes(held[pair, :, :, lanes], 0, 1)
            for e in range(2):
                for s in range(4):
                    ready[pair, s, e, :, lanes] = x[4 * e + s]
            return 0

        lax.fori_loop(0, ny // 128, tile, 0, unroll=4)
        copy = pltpu.make_async_copy(ready.at[pair], out.at[:, pl.ds(2 * pair, 2)], sems.at[pair])
        copy.start()
        copies.append(copy)
    flow_in.wait()
    flow_copy = pltpu.make_async_copy(held_flow, flow_out, sems.at[4])
    flow_copy.start()
    for copy in copies:
        copy.wait()
    flow_copy.wait()


def body(tracers, flow, reaction_rates, land_mask, layers):
    ny = tracers.shape[-1]
    vmem = pl.BlockSpec(memory_space=pltpu.VMEM)
    anywhere = pl.BlockSpec(memory_space=pl.ANY)
    dma = pltpu.SemaphoreType.DMA
    blocks, flow_done = pl.pallas_call(
        kernel,
        out_shape=(
            jax.ShapeDtypeStruct((4, ROWS, 8, ny), F32),
            jax.ShapeDtypeStruct((4, ROWS, ny), F32),
        ),
        in_specs=[pl.BlockSpec(memory_space=pltpu.HBM)] * 2 + [vmem] * 3,
        out_specs=(anywhere, anywhere),
        scratch_shapes=[
            pltpu.VMEM((4, 8, ROWS, ny), F32),
            pltpu.VMEM((4, ROWS, ny), F32),
            pltpu.VMEM((ROWS, ny), F32),
            pltpu.VMEM((32, 32), F32),
            pltpu.VMEM((4, 2, 4, ROWS, ny), F32),
            pltpu.VMEM((STEPS, 4, SPAN, 8, ny), F32),
            pltpu.VMEM((SPAN, 8, ny), F32),
            pltpu.VMEM((SPAN, 8, ny), F32),
            pltpu.VMEM((4, ROWS, 8, ny), F32),
            pltpu.VMEM((STEPS, 13, 4, 8, ny), F32),
            pltpu.VMEM((STEPS, 12, 4, 8, ny), F32),
            pltpu.VMEM((ROWS, 2, 8, ny), F32),
            pltpu.VMEM((2, 8, DEEP, ny), F32),
            pltpu.VMEM((STEPS + 1, 2, 2, DEEP, ny), F32),
            pltpu.VMEM((DEEP, ny), F32),
            pltpu.VMEM((STEPS, 4, 2, HALF, 8, ny), F32),
            pltpu.VMEM((STEPS, 2, 4, HALF, 8, ny), F32),
            pltpu.VMEM((4, ROWS, 8, ny), F32),
            pltpu.VMEM((2, 2, ROWS, ny), F32),
            dma((3,)), dma((3, 2, 2)), dma((4, 2, 2)),
            dma((2,)), dma((2,)), dma((2,)), dma((3,)), dma((3,)), dma((3,)), dma((3,)),
            dma((4, 4, 2)), dma((4, 4, 2)),
            dma((3, 4, 2)), dma((3, 4, 2)),
            dma((3, 3)), dma((4, 3)), dma((3,)),
            dma((2,)), dma((2,)), dma((1,)),
        ],
        compiler_params=pltpu.CompilerParams(
            collective_id=0, has_side_effects=True, vmem_limit_bytes=ALL_VMEM
        ),
        name="ocean",
    )(tracers, flow, reaction_rates, land_mask, layers)
    return pl.pallas_call(
        place,
        out_shape=(
            jax.ShapeDtypeStruct(tracers.shape, F32),
            jax.ShapeDtypeStruct(flow.shape, F32),
        ),
        in_specs=[pl.BlockSpec(memory_space=pltpu.HBM)] * 2,
        out_specs=(pl.BlockSpec(memory_space=pltpu.HBM),) * 2,
        scratch_shapes=[
            pltpu.VMEM((4, ROWS, 8, ny), F32),
            pltpu.VMEM((4, ROWS, ny), F32),
            pltpu.VMEM((4, 4, 2, ROWS, ny), F32),
            dma((10,)),
        ],
        compiler_params=pltpu.CompilerParams(vmem_limit_bytes=ALL_VMEM),
        name="place",
    )(blocks, flow_done)


def solution(mesh):
    placed = (
        P(("comp", "trc"), None, "space", None),
        P(("comp", "trc"), "space", None),
        P(),
        P("space", None),
        P("space", None),
    )
    return jax.shard_map(
        body,
        mesh=mesh,
        in_specs=placed,
        out_specs=(P(("comp", "trc"), None, "space", None), P(("comp", "trc"), "space", None)),
        check_vma=False,
    )
```

```python
import functools

import jax
import jax.numpy as jnp
from jax import lax
from jax.experimental import pallas as pl
from jax.experimental.pallas import tpu as pltpu
from jax.sharding import PartitionSpec as P

STEPS = 2
COURANT = 0.25
VISCOSITY = 0.2
CORIOLIS = 0.3
FRICTION = 0.1
DIFFUSION = 0.3
REACT_STEP = 0.5

MESH = pl.DeviceIdType.MESH
F32 = jnp.float32
ROWS = 8
DEEP = 24
GHOST = 4
SPAN = ROWS + 2 * GHOST
EDGE = 128
HALF = ROWS // 2
ALL_VMEM = 67_043_328
LINE = 8
PAIR = 128
PAIRS = 2


def limited(before, after):
    return jnp.maximum(jnp.minimum(after, 0.0), jnp.minimum(before, jnp.maximum(after, 0.0)))


def roll_lanes(a, by):
    return pltpu.roll(a, by % a.shape[-1], a.ndim - 1)


def kernel(
    tracers, flow, rates, land, layers, out, flow_out,
    tr_v, fl_v, dep_v, matrix, stage, grid, first, part, second, coef_x, coef_y, mix_w, natural,
    field, depth_v, packed, ext, final, velocity_send,
    in_local, in_sem_s, in_sem_r, fl_local, fl_sem_s, fl_sem_r, rel_s, rel_r, dep_s, dep_r,
    halo_s, halo_r, mix_s, mix_r, out_s, out_r, own_out, fo_s, fo_r, fo_own,
):
    ny = tracers.shape[-1]
    c = lax.axis_index("comp")
    sp = lax.axis_index("space")
    t = lax.axis_index("trc")
    n = lax.axis_size("space")
    w = 2 * c + t
    has_prev = sp > 0
    has_next = sp < n - 1

    def odd(strip):
        return lax.rem(strip // LINE + 1, 2)

    def flipped(bit, strip):
        return lax.rem(bit + odd(strip), 2)

    flip = odd(sp)
    tl = flipped(t, sp)
    v = 2 * tl + c

    def at(cc, ss, tt):
        return {"comp": cc, "space": ss, "trc": tt}

    def holder(pair, strip):
        return at(lax.rem(pair, 2), strip, flipped(pair // 2, strip))

    def remote(src, dst, s, r, dev):
        return pltpu.make_async_remote_copy(
            src_ref=src, dst_ref=dst, send_sem=s, recv_sem=r, device_id=dev, device_id_type=MESH
        )

    middle = pl.ds(ROWS, ROWS)
    mid = ny // 2
    cut = mid + EDGE
    width = mid + EDGE

    all_flow = pltpu.make_async_copy(flow, fl_v, fl_local.at[1])
    all_tr = pltpu.make_async_copy(tracers, tr_v, in_local.at[0])
    own_tr = [
        pltpu.make_async_copy(tracers.at[:, 2 * v + e], stage.at[w, e], in_local.at[1 + e])
        for e in range(2)
    ]
    my_flow = pltpu.make_async_copy(
        flow.at[pl.ds(2 * c, 2)], field.at[0, c, :, middle], fl_local.at[0]
    )
    all_flow.start()
    all_tr.start()
    for copy in own_tr:
        copy.start()

    @pl.when(flip == 0)
    def _():
        my_flow.start()

    barrier = pltpu.get_barrier_semaphore()
    peers = [(c, 1 - t), (1 - c, 1 - t), (1 - c, t)]

    def pair_of(cc, tt):
        return 2 * flipped(tt, sp) + cc

    for cc, tt in peers:
        pl.semaphore_signal(barrier, inc=1, device_id=at(cc, sp, tt), device_id_type=MESH)

    @pl.when(has_prev)
    def _():
        pl.semaphore_signal(barrier, inc=1, device_id=holder(v, sp - 1), device_id_type=MESH)

    @pl.when(has_next)
    def _():
        pl.semaphore_signal(barrier, inc=1, device_id=holder(v, sp + 1), device_id_type=MESH)

    dep_v[...] = jnp.where(land[...] > 0, layers[...], 0).astype(F32)
    depth_v[middle] = dep_v[...]

    @pl.when(jnp.logical_not(has_prev))
    def _():
        depth_v[0:ROWS] = jnp.zeros((ROWS, ny), F32)
        for comp in range(2):
            for e in range(2):
                field[0, comp, e, 0:ROWS] = jnp.zeros((ROWS, ny), F32)
        for step in range(2):
            for slot in range(4):
                for row in range(GHOST):
                    grid[step, slot, row] = jnp.zeros((8, ny), F32)

    @pl.when(jnp.logical_not(has_next))
    def _():
        depth_v[2 * ROWS :] = jnp.zeros((ROWS, ny), F32)
        for comp in range(2):
            for e in range(2):
                field[0, comp, e, 2 * ROWS :] = jnp.zeros((ROWS, ny), F32)
        for step in range(2):
            for slot in range(4):
                for row in range(GHOST):
                    grid[step, slot, GHOST + ROWS + row] = jnp.zeros((8, ny), F32)

    @pl.when(v == 0)
    def _():
        for step in range(2):
            for slot in range(4):
                ext[step, 0, slot] = jnp.zeros((HALF, 8, ny), F32)

    @pl.when(v == 3)
    def _():
        for step in range(2):
            for slot in range(4):
                ext[step, 1, slot] = jnp.zeros((HALF, 8, ny), F32)

    lines = lax.broadcasted_iota(jnp.int32, (32, 16), 0)
    names = lax.broadcasted_iota(jnp.int32, (32, 16), 1)
    pick = jnp.where(4 * (lines // 8) + lax.rem(lines, 4) == names, 1.0, 0.0)
    wide = jnp.dot(pick, rates[...], precision=lax.Precision.HIGHEST, preferred_element_type=F32)
    wide = lax.dot_general(
        wide, pick, (((1,), (1,)), ((), ())),
        precision=lax.Precision.HIGHEST, preferred_element_type=F32,
    )
    line = lax.broadcasted_iota(jnp.int32, (32, 32), 0)
    other = lax.broadcasted_iota(jnp.int32, (32, 32), 1)
    same_level = lax.rem(line // 4, 2) == lax.rem(other // 4, 2)
    matrix[...] = jnp.where(same_level, REACT_STEP * wide, 0.0)

    all_flow.wait()
    pl.semaphore_wait(barrier, 3 + jnp.where(has_prev, 1, 0) + jnp.where(has_next, 1, 0))

    def flow_copy(cc):
        return remote(
            fl_v.at[pl.ds(2 * cc, 2)], field.at[0, c, :, middle],
            fl_sem_s.at[cc], fl_sem_r.at[c], holder(2 * t + cc, sp),
        )

    def flow_from(cc):
        return remote(
            fl_v.at[pl.ds(0, 2)], field.at[0, cc, :, middle],
            fl_sem_s.at[cc], fl_sem_r.at[cc], at(cc, sp, tl),
        )

    @pl.when(flip == 0)
    def _():
        flow_copy(1 - c).start()

    @pl.when(flip == 1)
    def _():
        for cc in range(2):
            flow_copy(cc).start()

    def in_copy(k, side, e):
        cc, tt = peers[k]
        lanes = pl.ds(side * mid, mid)
        return remote(
            tr_v.at[:, 2 * pair_of(cc, tt) + e, :, lanes], stage.at[w, e, :, :, lanes],
            in_sem_s.at[k, side, e], in_sem_r.at[w, side, e], at(cc, sp, tt),
        )

    all_tr.wait()
    for k in (2, 0, 1):
        for side in range(2):
            for e in range(2):
                in_copy(k, side, e).start()

    def dep_copy(d):
        return remote(
            dep_v, depth_v.at[pl.ds(ROWS * (1 - d), ROWS)],
            dep_s.at[d + 1], dep_r.at[1 - d], holder(v, sp + d),
        )

    def relay_copy(d):
        return remote(
            field.at[0, :, :, middle], field.at[0, :, :, pl.ds(ROWS * (1 - d), ROWS)],
            rel_s.at[d + 1], rel_r.at[1 - d], holder(v, sp + d),
        )

    @pl.when(has_prev)
    def _():
        dep_copy(-1).start()

    @pl.when(has_next)
    def _():
        dep_copy(1).start()

    def halo_copy(wave, slot, d):
        low = d < 0
        step, lanes = (
            (0, pl.ds(0, mid)), (1, pl.ds(0, cut)), (1, pl.ds(cut, ny - cut)),
            (0, pl.ds(mid, ny - mid)),
        )[wave]
        return remote(
            grid.at[step, slot, pl.ds(GHOST if low else ROWS, GHOST), :, lanes],
            grid.at[step, slot, pl.ds(GHOST + ROWS if low else 0, GHOST), :, lanes],
            halo_s.at[wave, slot, 0 if low else 1], halo_r.at[wave, slot, 1 if low else 0],
            holder(v, sp + d),
        )

    def halo_start(wave, slot):
        @pl.when(has_prev)
        def _():
            halo_copy(wave, slot, -1).start()

        @pl.when(has_next)
        def _():
            halo_copy(wave, slot, 1).start()

    def halo_wait(wave, slot):
        @pl.when(has_prev)
        def _():
            halo_copy(wave, slot, 1).wait_recv()

        @pl.when(has_next)
        def _():
            halo_copy(wave, slot, -1).wait_recv()

    def halo_sent(wave, slot):
        @pl.when(has_prev)
        def _():
            halo_copy(wave, slot, -1).wait_send()

        @pl.when(has_next)
        def _():
            halo_copy(wave, slot, 1).wait_send()

    def regroup(slot, side):
        def tile(q, _):
            lanes = pl.ds(pl.multiple_of(q * 128, 128), 128)
            x = stage[slot, :, :, :, lanes].reshape(8, ROWS, 128)
            grid[0, slot, pl.ds(GHOST, ROWS), :, lanes] = jnp.swapaxes(x, 0, 1)
            return 0

        tiles = mid // 128
        lax.fori_loop(side * tiles, (side + 1) * tiles, tile, 0, unroll=2)

    def arrived(k):
        cc, tt = peers[k]
        slot = 2 * cc + tt
        for side in range(2):
            lanes = pl.ds(side * mid, mid)
            for e in range(2):
                remote(
                    stage.at[slot, e, :, :, lanes], stage.at[slot, e, :, :, lanes],
                    in_sem_s.at[k, side, e], in_sem_r.at[slot, side, e], at(cc, sp, tt),
                ).wait_recv()
            regroup(slot, side)
            halo_start(3 * side, slot)

    for copy in own_tr:
        copy.wait()
    for side in range(2):
        regroup(w, side)

    @pl.when(flip == 0)
    def _():
        my_flow.wait()
        flow_from(1 - c).wait_recv()

    @pl.when(flip == 1)
    def _():
        for cc in range(2):
            flow_from(cc).wait_recv()

    @pl.when(has_prev)
    def _():
        relay_copy(-1).start()

    @pl.when(has_next)
    def _():
        relay_copy(1).start()

    for side in range(2):
        halo_start(3 * side, w)
    arrived(2)

    @pl.when(has_prev)
    def _():
        dep_copy(1).wait_recv()
        relay_copy(1).wait_recv()

    @pl.when(has_next)
    def _():
        dep_copy(-1).wait_recv()
        relay_copy(-1).wait_recv()

    lane_deep = lax.broadcasted_iota(jnp.int32, (DEEP, ny), 1)
    top_half = lax.broadcasted_iota(jnp.int32, (8, ny), 0) < 4

    def wet_of(level, rows):
        return jnp.where(depth_v[rows] > level.astype(F32), 1.0, 0.0)

    def lap(a):
        left = jnp.where(lane_deep == 0, 0.0, roll_lanes(a, 1))
        right = jnp.where(lane_deep == ny - 1, 0.0, roll_lanes(a, -1))
        return pltpu.roll(a, 1, 0) + pltpu.roll(a, DEEP - 1, 0) + left + right - 4.0 * a

    def put_coefs(e, base, face):
        up = jnp.maximum(face, 0.0)
        down = jnp.minimum(face, 0.0)
        natural[e, base] = -COURANT * up
        natural[e, base + 1] = (-COURANT * 0.5) * up * (1.0 - COURANT * up)
        natural[e, base + 2] = -COURANT * down
        natural[e, base + 3] = (COURANT * 0.5) * down * (1.0 + COURANT * down)

    def spread_rows(ref, k, j):
        one = jnp.broadcast_to(ref[0, k, j : j + 1, :], (8, ny))
        two = jnp.broadcast_to(ref[1, k, j : j + 1, :], (8, ny))
        return jnp.where(top_half, one, two)

    def velocities(step, _):
        def level(e, _):
            wet = wet_of(2 * v + e, slice(None))
            u = field[step, 0, e]
            r = field[step, 1, e]
            u_new = wet * (u + CORIOLIS * r + VISCOSITY * lap(u) - FRICTION * u)
            r_new = wet * (r - CORIOLIS * u + VISCOSITY * lap(r) - FRICTION * r)
            field[step + 1, 0, e] = u_new
            field[step + 1, 1, e] = r_new
            face = 0.5 * (u_new + pltpu.roll(u_new, DEEP - 1, 0)) * wet * pltpu.roll(wet, DEEP - 1, 0)
            put_coefs(e, 0, face)
            wet_right = jnp.where(lane_deep == ny - 1, 0.0, roll_lanes(wet, -1))
            face = 0.5 * (r_new + roll_lanes(r_new, -1)) * wet * wet_right
            put_coefs(e, 4, face)
            return 0

        lax.fori_loop(0, 2, level, 0)
        shift = ROWS - GHOST
        for i in range(1, 14):
            for k in range(4):
                coef_x[step, i - 1, k] = spread_rows(natural, k, i + shift)
        for i in range(2, 14):
            for k in range(4):
                coef_y[step, i - 2, k] = spread_rows(natural, 4 + k, i + shift)
        return 0

    velocities(0, 0)

    def velocity_copy(comp):
        return remote(
            velocity_send.at[comp], flow_out.at[pl.ds(2 * c, 2)],
            fo_s.at[comp], fo_r.at[c], at(comp, sp, tl),
        )

    def velocity_from(cc):
        return remote(
            velocity_send.at[0], flow_out.at[pl.ds(2 * cc, 2)],
            fo_s.at[0], fo_r.at[cc], holder(2 * t + cc, sp),
        )

    velocity_own = pltpu.make_async_copy(
        velocity_send.at[c], flow_out.at[pl.ds(2 * c, 2)], fo_own.at[0]
    )

    own_rows = slice(ROWS, 2 * ROWS)

    def mixing_weights():
        above = jnp.where(v > 0, DIFFUSION, 0.0).astype(F32)
        wet_a = wet_of(2 * v, own_rows)
        wet_b = wet_of(2 * v + 1, own_rows)
        natural[0, 0, 0:ROWS] = DIFFUSION * wet_a * wet_b
        natural[1, 0, 0:ROWS] = DIFFUSION * wet_a * wet_b
        natural[0, 1, 0:ROWS] = above * wet_a * wet_of(2 * v - 1, own_rows)
        natural[1, 1, 0:ROWS] = DIFFUSION * wet_b * wet_of(2 * v + 2, own_rows)
        for row in range(ROWS):
            for k in range(2):
                mix_w[row, k] = spread_rows(natural, k, row)


    def send_velocities():
        for comp in range(2):
            for e in range(2):
                velocity_send[comp, e] = field[STEPS, comp, e, own_rows]

        @pl.when(flip == 0)
        def _():
            velocity_own.start()
            velocity_copy(1 - c).start()

        @pl.when(flip == 1)
        def _():
            for comp in range(2):
                velocity_copy(comp).start()

    def along_x(step, load, first_face, last_face, start, size, put):
        def chunk(q, _):
            lanes = pl.ds(pl.multiple_of(start + q * PAIR, 128), PAIR)
            before = load(first_face - 1, lanes)
            here = load(first_face, lanes)
            ahead = load(first_face + 1, lanes)
            jump = ahead - here
            slope = limited(here - before, jump)
            last_flux = None
            for i in range(first_face, last_face + 1):
                far = load(i + 2, lanes)
                next_jump = far - ahead
                next_slope = limited(jump, next_jump)
                k = i - 1
                flux = (
                    coef_x[step, k, 0, :, lanes] * here
                    + coef_x[step, k, 1, :, lanes] * slope
                    + coef_x[step, k, 2, :, lanes] * ahead
                    + coef_x[step, k, 3, :, lanes] * next_slope
                )
                if last_flux is not None:
                    put(i, lanes, here, flux - last_flux)
                last_flux = flux
                here, ahead, jump, slope = ahead, far, next_jump, next_slope
            return 0

        lax.fori_loop(0, size // PAIR, chunk, 0, unroll=PAIRS)

    def along_y(step, i, a, lanes):
        columns = lax.broadcasted_iota(jnp.int32, a.shape, 1)
        right = jnp.where(columns == a.shape[1] - 1, 0.0, roll_lanes(a, -1))
        jump = right - a
        slope = limited(jnp.where(columns == 0, a, roll_lanes(jump, 1)), jump)
        flux = (
            coef_y[step, i - 2, 0, :, lanes] * a
            + coef_y[step, i - 2, 1, :, lanes] * slope
            + coef_y[step, i - 2, 2, :, lanes] * right
            + coef_y[step, i - 2, 3, :, lanes] * roll_lanes(slope, -1)
        )
        return flux - jnp.where(columns == 0, 0.0, roll_lanes(flux, 1))

    def advance(step, slot, start, size, keep_start, keep_size):
        lanes = pl.ds(start, size)
        kept = pl.ds(keep_start, keep_size)
        skip = keep_start - start

        def put_one(i, at_lanes, here, change):
            part[i, :, at_lanes] = here + change

        along_x(
            step, lambda i, at_lanes: grid[step, slot, i, :, at_lanes], 1, 13, start, size, put_one
        )

        def row_one(i, _):
            first[i, :, lanes] = part[i, :, lanes] + along_y(
                step, i, grid[step, slot, i, :, lanes], lanes
            )
            return 0

        lax.fori_loop(2, 14, row_one, 0, unroll=True)

        def put_two(i, at_lanes, here, change):
            part[i, :, at_lanes] = (grid[step, slot, i, :, at_lanes] + here) + change

        along_x(
            step, lambda i, at_lanes: first[i, :, at_lanes], 3, 11, keep_start, keep_size, put_two
        )

        def row_two(i, _):
            change = along_y(step, i, first[i, :, lanes], lanes)
            second[slot, i - GHOST, :, kept] = 0.5 * (
                part[i, :, kept] + change[:, skip : skip + keep_size]
            )
            return 0

        lax.fori_loop(GHOST, GHOST + ROWS, row_two, 0, unroll=True)

    def swap_halves(a):
        return pltpu.roll(a, 4, 0)

    kept_of = ((0, ny), (0, mid), (mid, ny - mid))

    def mix_copy(wave, slot, d):
        step, lanes = min(wave, 1), pl.ds(*kept_of[wave])
        return remote(
            packed.at[step, slot, 0 if d < 0 else 1, :, :, lanes],
            ext.at[step, 1 if d < 0 else 0, slot, :, :, lanes],
            mix_s.at[wave, slot, 0 if d < 0 else 1], mix_r.at[wave, slot, 1 if d < 0 else 0],
            holder(v + d, sp),
        )

    def mix_start(wave, slot):
        step, lanes = min(wave, 1), pl.ds(*kept_of[wave])
        in_top = lax.broadcasted_iota(jnp.int32, (8, kept_of[wave][1]), 0) < 4

        def row(i, _):
            a = second[slot, i, :, lanes]
            b = second[slot, i + HALF, :, lanes]
            packed[step, slot, 0, i, :, lanes] = jnp.where(in_top, a, swap_halves(b))
            packed[step, slot, 1, i, :, lanes] = jnp.where(in_top, swap_halves(a), b)
            return 0

        lax.fori_loop(0, HALF, row, 0, unroll=True)

        @pl.when(v > 0)
        def _():
            mix_copy(wave, slot, -1).start()

        @pl.when(v < 3)
        def _():
            mix_copy(wave, slot, 1).start()

    def mix_wait(wave, slot):
        @pl.when(v > 0)
        def _():
            mix_copy(wave, slot, 1).wait_recv()

        @pl.when(v < 3)
        def _():
            mix_copy(wave, slot, -1).wait_recv()

    def mix_sent(wave, slot):
        @pl.when(v > 0)
        def _():
            mix_copy(wave, slot, -1).wait_send()

        @pl.when(v < 3)
        def _():
            mix_copy(wave, slot, 1).wait_send()

    def settle(step, put, start, size):
        lanes = pl.ds(start, size)
        in_top = lax.broadcasted_iota(jnp.int32, (8, size), 0) < 4

        def reacted(i, beyond_of):
            inner = mix_w[i, 0, :, lanes]
            outer = mix_w[i, 1, :, lanes]
            mixed = []
            for slot in range(4):
                a = second[slot, i, :, lanes]
                beyond = beyond_of(slot)
                mixed.append(a + inner * (swap_halves(a) - a) + outer * (beyond - a))
            whole = jnp.concatenate(mixed, axis=0)
            soft = whole / (1.0 + jnp.abs(whole))
            done = whole + jnp.dot(
                matrix[...], soft, precision=lax.Precision.HIGHEST, preferred_element_type=F32
            )
            for slot in range(4):
                put(slot, i, lanes, done[8 * slot : 8 * slot + 8])

        def rows(j, _):
            reacted(
                j,
                lambda slot: jnp.where(
                    in_top,
                    ext[step, 0, slot, j, :, lanes],
                    swap_halves(ext[step, 1, slot, j, :, lanes]),
                ),
            )
            reacted(
                j + HALF,
                lambda slot: jnp.where(
                    in_top,
                    swap_halves(ext[step, 0, slot, j, :, lanes]),
                    ext[step, 1, slot, j, :, lanes],
                ),
            )
            return 0

        lax.fori_loop(0, HALF, rows, 0, unroll=2)

    between = jnp.logical_or(
        jnp.logical_and(has_prev, odd(sp - 1) != flip),
        jnp.logical_and(has_next, odd(sp + 1) != flip),
    )
    near, far, last = 2 * (1 - c) + t, 2 * c + 1 - t, 2 * (1 - c) + 1 - t
    order = [
        jnp.where(between, far, w), jnp.where(between, last, near), jnp.where(between, w, far),
        jnp.where(between, near, last),
    ]

    arrived(0)

    @pl.when(between)
    def _():
        arrived(1)

    for number, slot in enumerate(order):
        if number == 2:

            @pl.when(jnp.logical_not(between))
            def _():
                arrived(1)

        if number == 3:
            velocities(1, 0)
        halo_wait(0, slot)
        halo_wait(3, slot)
        advance(0, slot, 0, ny, 0, ny)
        mix_start(0, slot)
    mixing_weights()
    for slot in range(4):
        mix_wait(0, slot)

    def put_next(slot, i, lanes, a):
        grid[1, slot, GHOST + i, :, lanes] = a

    for wave, (start, size) in ((1, (0, cut)), (2, (cut, ny - cut))):
        settle(0, put_next, start, size)
        for slot in range(4):
            halo_start(wave, slot)

    send_velocities()

    def put_final(slot, i, lanes, a):
        final[slot, i, :, lanes] = a

    def out_copy(k, wave):
        cc, tt = peers[k]
        lanes = pl.ds(*kept_of[wave])
        return remote(
            final.at[2 * cc + tt, :, :, lanes], out.at[v, :, :, lanes],
            out_s.at[k, wave], out_r.at[v, wave], at(cc, sp, tt),
        )

    def out_from(k, wave):
        cc, tt = peers[k]
        lanes = pl.ds(*kept_of[wave])
        source = pair_of(cc, tt)
        return remote(
            final.at[w, :, :, lanes], out.at[source, :, :, lanes],
            out_s.at[k, wave], out_r.at[source, wave], at(cc, sp, tt),
        )

    def own_copy(wave):
        lanes = pl.ds(*kept_of[wave])
        return pltpu.make_async_copy(
            final.at[w, :, :, lanes], out.at[v, :, :, lanes], own_out.at[wave]
        )

    def window(wave, slots):
        def one(slot, _):
            halo_wait(wave, slot)
            start = (0, ny - width)[wave - 1]
            advance(1, slot, start, width, *kept_of[wave])
            mix_start(wave, slot)
            return 0

        lax.fori_loop(*slots, one, 0)

    def finish(wave):
        for slot in range(4):
            mix_wait(wave, slot)
        settle(1, put_final, *kept_of[wave])
        for k in range(3):
            out_copy(k, wave).start()
        own_copy(wave).start()

    window(1, (0, 4))
    window(2, (0, 4))
    finish(1)
    finish(2)

    for wave in (1, 2):
        own_copy(wave).wait()

    @pl.when(flip == 0)
    def _():
        velocity_own.wait()
        velocity_copy(1 - c).wait_send()
        velocity_from(1 - c).wait_recv()
        flow_copy(1 - c).wait_send()

    @pl.when(flip == 1)
    def _():
        for cc in range(2):
            velocity_copy(cc).wait_send()
            velocity_from(cc).wait_recv()
            flow_copy(cc).wait_send()

    for k in range(3):
        for side in range(2):
            for e in range(2):
                in_copy(k, side, e).wait_send()

    @pl.when(has_prev)
    def _():
        dep_copy(-1).wait_send()
        relay_copy(-1).wait_send()

    @pl.when(has_next)
    def _():
        dep_copy(1).wait_send()
        relay_copy(1).wait_send()

    for slot in range(4):
        for wave in range(4):
            halo_sent(wave, slot)
        for wave in range(3):
            mix_sent(wave, slot)
    for wave in (1, 2):
        for k in range(3):
            out_copy(k, wave).wait_send()
            out_from(k, wave).wait_recv()


def place(blocks, flow, out, flow_out, held, held_flow, ready, sems):
    ny = blocks.shape[-1]
    loads = [pltpu.make_async_copy(blocks.at[g], held.at[g], sems.at[5 + g]) for g in range(4)]
    for load in loads:
        load.start()
    flow_in = pltpu.make_async_copy(flow, held_flow, sems.at[9])
    flow_in.start()
    copies = []
    for pair in range(4):
        loads[pair].wait()

        def tile(q, _):
            lanes = pl.ds(pl.multiple_of(q * 128, 128), 128)
            x = jnp.swapaxes(held[pair, :, :, lanes], 0, 1)
            for e in range(2):
                for s in range(4):
                    ready[pair, s, e, :, lanes] = x[4 * e + s]
            return 0

        lax.fori_loop(0, ny // 128, tile, 0, unroll=4)
        copy = pltpu.make_async_copy(ready.at[pair], out.at[:, pl.ds(2 * pair, 2)], sems.at[pair])
        copy.start()
        copies.append(copy)
    flow_in.wait()
    flow_copy = pltpu.make_async_copy(held_flow, flow_out, sems.at[4])
    flow_copy.start()
    for copy in copies:
        copy.wait()
    flow_copy.wait()


def body(tracers, flow, reaction_rates, land_mask, layers):
    ny = tracers.shape[-1]
    vmem = pl.BlockSpec(memory_space=pltpu.VMEM)
    anywhere = pl.BlockSpec(memory_space=pl.ANY)
    dma = pltpu.SemaphoreType.DMA
    blocks, flow_done = pl.pallas_call(
        kernel,
        out_shape=(
            jax.ShapeDtypeStruct((4, ROWS, 8, ny), F32),
            jax.ShapeDtypeStruct((4, ROWS, ny), F32),
        ),
        in_specs=[pl.BlockSpec(memory_space=pltpu.HBM)] * 2 + [vmem] * 3,
        out_specs=(anywhere, anywhere),
        scratch_shapes=[
            pltpu.VMEM((4, 8, ROWS, ny), F32),
            pltpu.VMEM((4, ROWS, ny), F32),
            pltpu.VMEM((ROWS, ny), F32),
            pltpu.VMEM((32, 32), F32),
            pltpu.VMEM((4, 2, 4, ROWS, ny), F32),
            pltpu.VMEM((STEPS, 4, SPAN, 8, ny), F32),
            pltpu.VMEM((SPAN, 8, ny), F32),
            pltpu.VMEM((SPAN, 8, ny), F32),
            pltpu.VMEM((4, ROWS, 8, ny), F32),
            pltpu.VMEM((STEPS, 13, 4, 8, ny), F32),
            pltpu.VMEM((STEPS, 12, 4, 8, ny), F32),
            pltpu.VMEM((ROWS, 2, 8, ny), F32),
            pltpu.VMEM((2, 8, DEEP, ny), F32),
            pltpu.VMEM((STEPS + 1, 2, 2, DEEP, ny), F32),
            pltpu.VMEM((DEEP, ny), F32),
            pltpu.VMEM((STEPS, 4, 2, HALF, 8, ny), F32),
            pltpu.VMEM((STEPS, 2, 4, HALF, 8, ny), F32),
            pltpu.VMEM((4, ROWS, 8, ny), F32),
            pltpu.VMEM((2, 2, ROWS, ny), F32),
            dma((3,)), dma((3, 2, 2)), dma((4, 2, 2)),
            dma((2,)), dma((2,)), dma((2,)), dma((3,)), dma((3,)), dma((3,)), dma((3,)),
            dma((4, 4, 2)), dma((4, 4, 2)),
            dma((3, 4, 2)), dma((3, 4, 2)),
            dma((3, 3)), dma((4, 3)), dma((3,)),
            dma((2,)), dma((2,)), dma((1,)),
        ],
        compiler_params=pltpu.CompilerParams(
            collective_id=0, has_side_effects=True, vmem_limit_bytes=ALL_VMEM
        ),
        name="ocean",
    )(tracers, flow, reaction_rates, land_mask, layers)
    return pl.pallas_call(
        place,
        out_shape=(
            jax.ShapeDtypeStruct(tracers.shape, F32),
            jax.ShapeDtypeStruct(flow.shape, F32),
        ),
        in_specs=[pl.BlockSpec(memory_space=pltpu.HBM)] * 2,
        out_specs=(pl.BlockSpec(memory_space=pltpu.HBM),) * 2,
        scratch_shapes=[
            pltpu.VMEM((4, ROWS, 8, ny), F32),
            pltpu.VMEM((4, ROWS, ny), F32),
            pltpu.VMEM((4, 4, 2, ROWS, ny), F32),
            dma((10,)),
        ],
        compiler_params=pltpu.CompilerParams(vmem_limit_bytes=ALL_VMEM),
        name="place",
    )(blocks, flow_done)


def solution(mesh):
    placed = (
        P(("comp", "trc"), None, "space", None),
        P(("comp", "trc"), "space", None),
        P(),
        P("space", None),
        P("space", None),
    )
    return jax.shard_map(
        body,
        mesh=mesh,
        in_specs=placed,
        out_specs=(P(("comp", "trc"), None, "space", None), P(("comp", "trc"), "space", None)),
        check_vma=False,
    )
```
